256 devices in a mesh: ea: 64 (over z, x, core), sa: 4 (over y).
Axes of the slice: x: 4, y: 4, z: 8, core: 2. Of those that a mesh axis runs over, the one named last changes fastest.
Arguments:
- expert_hidden: bfloat16 [256, 1792, 512], P('ea', 'sa'), may hold values from -6 to 6
- down_weight: bfloat16 [256, 512, 2048], P('ea'), may hold values from -0.25 to 0.25
- residual: bfloat16 [64, 512, 2048], P('ea', 'sa'), may hold values from -6 to 6
- expert_ids: int32 [64, 512, 10], P('ea', 'sa'), may hold values from 0 to 255, all different within a row; in each aligned block of 128 rows (0 to 127, 128 to 255, ..., all dimensions but the last counted through in order) at most 7 rows name the same one
- combine_weight: float32 [64, 512, 10], P('ea', 'sa'), may hold values from 0.05 to 0.3
- norm_gain: bfloat16 [2048], replicated, may hold values from 0.25 to 1.75
- value_weight: bfloat16 [2048, 2048], P('ea'), may hold values from -0.125 to 0.125
- queries: bfloat16 [64, 512, 1024], P('ea', 'sa'), may hold values from -6 to 6
- keys: bfloat16 [64, 512, 1024], P('ea', 'sa'), may hold values from -6 to 6
- log_decay: float32 [64, 512, 16], P('ea', 'sa'), may hold values from -1 to 0, as said below
- write_rate: float32 [64, 512, 16], P('ea', 'sa'), may hold values from 0.1 to 0.9
Outputs:
- head_out: bfloat16 [64, 512, 2048], P('ea', 'sa')
The draws below stay inside these ranges and needn't reach their ends.
Inputs may be any that keep to these rules, and one draw needn't show every extreme that they name: `expert_ids`: each row names 10 different experts; among the rows of one device (aligned blocks of 128 rows) no expert is named more than 7 times, a bound that some block reaches. `log_decay`: below zero.
All inputs are finite; a program needn't handle non-finite values.
Results may differ from the reference program's by a relative error of at most 0.0066.
Values may be sent and summed in bfloat16 or wider, within the bound.
A program may use at most 128 MiB of HBM per device.

```python
import math
import jax
import jax.numpy as jnp
import numpy as np
from jax import lax

D = 2048
FF = 512
TOP = 10
HV = 16
HK = 8
DK = 128
DV = 128
TOK_DEV = 128
EXPERTS = 256
SEQS = 64
LEN = 512
CAP = 7
N_EA = 64
N_SA = 4


def draw_log_decay(key, part):
    k_fast, k_jitter, k_spots, k_drop = jax.random.split(key, 4)
    share = 0.5
    fast = jax.random.uniform(k_fast, (HV,)) < share
    slow_rate = 0.25 * math.log(10.0) / LEN
    base = jnp.where(fast, 1.0 / 40.0, slow_rate)
    jitter = jnp.exp(jax.random.uniform(k_jitter, (SEQS, LEN, HV), minval=-0.7, maxval=0.7))
    spots = jax.random.randint(k_spots, (SEQS, 2), 0, LEN)
    marked = jnp.any(jnp.arange(LEN)[None, :, None] == spots[:, None, :], axis=-1)
    drop = jnp.log(jax.random.uniform(k_drop, (SEQS, LEN), minval=0.5, maxval=0.8))
    final_result = -base[None, None, :] * jitter + jnp.where(marked, drop, 0.0)[:, :, None]
    return final_result.astype(jnp.float32)


def shard_levels(key, extent, pieces, smallest, top_value):
    level = 1.0
    for axis_at, parts in pieces:
        heights = jax.random.uniform(jax.random.fold_in(jax.random.fold_in(key, 6), axis_at), (parts,), jnp.float32, smallest / len(pieces), top_value / len(pieces))
        level = level * jnp.repeat(jnp.exp(heights), extent[axis_at] // parts).reshape((-1,) + (1,) * (len(extent) - 1 - axis_at))
    return level


def assign_block(own_key, own, number, rows, count, top, bound, lean):
    ranking = jax.random.permutation(own_key, count)
    crowded, ordinary = load_shares(count, rows * top, bound, lean, True), load_shares(count, rows * top, bound, lean, False)
    places = jnp.arange(count)

    def named(lengths, turn):
        used = int((lengths > 0).sum())
        fixed = max(1, used // 4)
        moved = fixed + (places - fixed + turn * (used - fixed)) % max(1, count - fixed)
        return jnp.zeros((count,), jnp.int32).at[ranking[jnp.where(places < fixed, places, moved)]].set(jnp.asarray(lengths, jnp.int32))

    lengths = jnp.where(number % 4 == 0, named(crowded, number // 4), named(ordinary, number - number // 4 - 1))
    mixed = jax.random.permutation(jax.random.fold_in(own, 3), count)
    source_of, receiver = mixed[0:count // 2 * 2:2], mixed[1:count // 2 * 2:2]
    room = jnp.minimum(lengths[source_of] - 1, bound - lengths[receiver]) // 2
    room = jnp.where((source_of == ranking[0]) | (receiver == ranking[0]) | (lengths[receiver] == 0), 0, jnp.maximum(room, 0))
    moved = jax.random.randint(jax.random.fold_in(own, 4), (count // 2,), 0, 1 << 20) % (room + 1)
    lengths = lengths.at[source_of].add(-moved).at[receiver].add(moved)
    members = jnp.searchsorted(jnp.cumsum(lengths), jnp.arange(rows * top), side="right").astype(jnp.int32)
    table = members.reshape(top, rows).T
    table = table[jax.random.permutation(jax.random.fold_in(own, 1), rows)]
    turn = jax.random.randint(jax.random.fold_in(own, 2), (rows, 1), 0, top)
    return jnp.take_along_axis(table, (jnp.arange(top)[None, :] + turn) % top, axis=1)


def load_shares(amount, total, limit, skew, full):
    portions = [(1 << 20) // math.isqrt(standing ** skew) + 1 for standing in range(1, amount + 1)]
    largest = limit if full else min(limit, max(-(-total // amount), total * portions[0] // sum(portions)))
    least = 1 if total - largest >= amount - 1 else 0
    given, spare = [largest] + [least] * (amount - 1), total - largest - least * (amount - 1)
    while spare > 0:
        movable = [i for i in range(1, amount) if given[i] < largest] or [i for i in range(1, amount) if given[i] < limit]
        pool, left = sum([portions[i] for i in movable]), spare
        for i in movable:
            extra = min(limit - given[i], max(1, left * portions[i] // pool), spare)
            given[i] = given[i] + extra
            spare = spare - extra
    return np.array(given)


def scatter_about(stream_key, extent, width, bound, cuts=(), kind=jnp.bfloat16):
    values = jax.random.normal(stream_key, extent, jnp.float32) * width
    if len(cuts) > 0:
        values = shard_levels(stream_key, extent, cuts, -0.22, 0.18) * values
    return jnp.clip(values, min=-bound, max=bound).astype(kind)


def setup_inputs(seed: int = 0) -> dict:
    key_of = jax.random.split(jax.random.key(seed), 12)
    expert_hidden = scatter_about(key_of[0], (EXPERTS, N_SA * N_EA * CAP, FF), 1.0, 6.0, ((0, 64), (1, 4)))
    down_weight = scatter_about(key_of[1], (EXPERTS, FF, D), FF ** -0.5, 0.25, ((0, 64),))
    residual = scatter_about(key_of[2], (SEQS, LEN, D), 1.0, 6.0, ((0, 64), (1, 4)))
    expert_ids_keys = jax.random.split(jax.random.fold_in(key_of[3], 1), SEQS * LEN // TOK_DEV)
    expert_ids_turns = jax.random.permutation(jax.random.fold_in(key_of[3], 3), SEQS * LEN // TOK_DEV)
    expert_ids = jax.vmap(lambda own, number: assign_block(jax.random.fold_in(key_of[3], 2), own, number, TOK_DEV, EXPERTS, TOP, CAP, 1))(expert_ids_keys, expert_ids_turns).reshape((SEQS, LEN, TOP))
    combine_weight = jnp.clip(0.05 + 0.25 * jax.random.uniform(key_of[4], (SEQS, LEN, TOP), jnp.float32) ** shard_levels(key_of[4], (SEQS, LEN, TOP), ((0, 64), (1, 4)), -0.2, 0.2), 0.05, 0.3)
    norm_gain = jnp.clip(1.0 + 0.15 * jax.random.normal(key_of[5], (D,), jnp.float32), 0.25, 1.75).astype(jnp.bfloat16)
    value_weight = scatter_about(key_of[6], (D, HV * DV), D ** -0.5, 0.125, ((0, 64),))
    queries = scatter_about(key_of[7], (SEQS, LEN, HK * DK), 1.0, 6.0, ((0, 64), (1, 4)))
    keys = scatter_about(key_of[8], (SEQS, LEN, HK * DK), 1.0, 6.0, ((0, 64), (1, 4)))
    log_decay = draw_log_decay(jax.random.fold_in(key_of[11], 71), 0)
    write_rate = jnp.clip(0.1 + 0.79999997 * jax.random.uniform(key_of[10], (SEQS, LEN, HV), jnp.float32) ** shard_levels(key_of[10], (SEQS, LEN, HV), ((0, 64), (1, 4)), -0.2, 0.2), 0.1, 0.9)
    return dict(expert_hidden=expert_hidden, down_weight=down_weight, residual=residual, expert_ids=expert_ids, combine_weight=combine_weight, norm_gain=norm_gain, value_weight=value_weight, queries=queries, keys=keys, log_decay=log_decay, write_rate=write_rate)


PRECISION_LEVEL = lax.Precision.HIGHEST

def block_slots(ids):
    onehot = (ids[:, :, None] == jnp.arange(EXPERTS, dtype=jnp.int32)[None, None, :]).astype(jnp.int32)
    counts = lax.optimization_barrier(jnp.sum(onehot, axis=1))
    prior = jnp.cumsum(counts, axis=0) - counts
    return lax.optimization_barrier(jnp.sum(onehot * prior[:, None, :], axis=-1)).astype(jnp.int32)

def unit_rows(field):
    return field * lax.rsqrt(lax.optimization_barrier(jnp.sum(field * field, axis=-1, keepdims=True)) + 1e-06)

def reference(expert_hidden, down_weight, residual, expert_ids, combine_weight, norm_gain, value_weight, queries, keys, log_decay, write_rate):
    down32 = down_weight.astype(jnp.float32)
    hidden5 = expert_hidden.reshape(EXPERTS, N_SA, N_EA, CAP, FF)
    per_seq = jnp.moveaxis(hidden5, 2, 0)

    def one_sequence(inputs):
        hid_seq, res_seq, ids_seq, weight_seq = inputs
        outs = jnp.einsum('ejcf,efd->ejcd', hid_seq.astype(jnp.float32), down32)
        flat = outs.reshape(EXPERTS * N_SA * CAP, D).astype(jnp.bfloat16)
        flat = lax.optimization_barrier(flat)
        ids_blocks = ids_seq.reshape(N_SA, TOK_DEV, TOP)
        slots = jax.vmap(block_slots)(ids_blocks)
        shard = jnp.arange(N_SA, dtype=jnp.int32)[:, None, None]
        rows = ((ids_blocks * N_SA + shard) * CAP + slots).reshape(LEN, TOP)
        picked = jnp.take(flat, rows, axis=0).astype(jnp.float32)
        moe = lax.optimization_barrier(jnp.sum(weight_seq[:, :, None] * picked, axis=1))
        return (res_seq.astype(jnp.float32) + moe).astype(jnp.bfloat16)
    stream = lax.map(one_sequence, (per_seq, residual, expert_ids, combine_weight))
    flow_float32 = lax.optimization_barrier(stream).astype(jnp.float32)
    normed = flow_float32 * lax.rsqrt(lax.optimization_barrier(jnp.mean(flow_float32 * flow_float32, axis=-1, keepdims=True)) + 1e-06) * norm_gain.astype(jnp.float32)
    normed = normed.astype(jnp.bfloat16)
    values = jnp.dot(normed.reshape(SEQS * LEN, D), value_weight, preferred_element_type=jnp.float32).astype(jnp.bfloat16)
    values = lax.optimization_barrier(values).astype(jnp.float32).reshape(SEQS, LEN, HV, DV)
    qn = unit_rows(queries.astype(jnp.float32).reshape(SEQS, LEN, HK, DK)) * DK ** (-0.5)
    kn = unit_rows(keys.astype(jnp.float32).reshape(SEQS, LEN, HK, DK))
    qn = jnp.repeat(qn, HV // HK, axis=2)
    kn = jnp.repeat(kn, HV // HK, axis=2)

    def advance(running_state, inputs):
        qt, kt, vt, at, bt = inputs
        alpha = jnp.exp(at)
        seen = jnp.einsum('shkv,shk->shv', running_state, kt, precision=PRECISION_LEVEL)
        delta = bt[..., None] * (vt - alpha[..., None] * seen)
        running_state = alpha[..., None, None] * running_state + kt[..., :, None] * delta[..., None, :]
        return (running_state, jnp.einsum('shkv,shk->shv', running_state, qt, precision=PRECISION_LEVEL))
    start = jnp.zeros((SEQS, HV, DK, DV), jnp.float32)
    inputs = (jnp.moveaxis(qn, 1, 0), jnp.moveaxis(kn, 1, 0), jnp.moveaxis(values, 1, 0), jnp.moveaxis(log_decay, 1, 0), jnp.moveaxis(write_rate, 1, 0))
    final, outs = lax.scan(advance, start, inputs)
    return jnp.moveaxis(outs, 0, 1).reshape(SEQS, LEN, HV * DV).astype(jnp.bfloat16)
```

```python
import jax
import jax.numpy as jnp
from jax import lax
from jax.experimental import pallas as pl
from jax.experimental.pallas import tpu as pltpu
from jax.sharding import PartitionSpec as P

HV = 16
HK = 8
DK = 128
DV = 128
BF = jnp.bfloat16
F32 = jnp.float32


def mm(a, b, dims=((1,), (0,))):
    return lax.dot_general(a.astype(BF), b.astype(BF), (dims, ((), ())), preferred_element_type=F32)


def mm_full(a, b, dims=((1,), (0,))):
    return lax.dot_general(
        a, b, (dims, ((), ())), preferred_element_type=F32, precision=lax.Precision.HIGHEST
    )


def mm3(a, b):
    ah, bh = a.astype(BF), b.astype(BF)
    al = (a - ah.astype(F32)).astype(BF)
    bl = (b - bh.astype(F32)).astype(BF)
    return mm(ah, bh) + (mm(ah, bl) + mm(al, bh))


def unit_lower_inverses(lowers):
    n = lowers[0].shape[0]
    row = lax.broadcasted_iota(jnp.int32, (n, n), 0)
    col = lax.broadcasted_iota(jnp.int32, (n, n), 1)
    eye = (row == col).astype(F32)
    size = 16
    same = (row // size) == (col // size)
    powers = [jnp.where(same, -low, 0.0) for low in lowers]
    outs = [eye + p for p in powers]
    for _ in range(3):
        powers = [mm3(p, p) for p in powers]
        outs = [o + mm3(p, o) for p, o in zip(powers, outs)]
    while size < n:
        join = ((row // (2 * size)) == (col // (2 * size))) & ((row // size) > (col // size))
        parts = [mm3(jnp.where(join, low, 0.0), o) for low, o in zip(lowers, outs)]
        outs = [o - mm3(o, p) for o, p in zip(outs, parts)]
        size *= 2
    return outs


def prepare_kernel(q_ref, k_ref, sum_ref, rate_ref, sumt_ref, ratet_ref, mbo_ref, a_ref, g_ref, *, pairs):
    n = q_ref.shape[0]
    row = lax.broadcasted_iota(jnp.int32, (n, n), 0)
    col = lax.broadcasted_iota(jnp.int32, (n, n), 1)
    inclusive = row >= col
    strict = row > col
    eye = (row == col).astype(F32)
    ones = jnp.ones((8, DK), F32)
    base = pl.program_id(0) * (2 * pairs)
    lane = lax.broadcasted_iota(jnp.int32, (n, HV), 1)
    heads, lowers = [], []
    for pair in range(pairs):
        q = q_ref[:, pair * DK : (pair + 1) * DK]
        k = k_ref[:, pair * DK : (pair + 1) * DK]
        qf, kf = q.astype(F32), k.astype(F32)
        kn_col = lax.rsqrt(jnp.sum(kf * kf, axis=-1, keepdims=True) + 1e-06)
        qn_col = lax.rsqrt(jnp.sum(qf * qf, axis=-1, keepdims=True) + 1e-06) * DK ** (-0.5)
        kn_row = lax.rsqrt(mm_full(ones, kf * kf, ((1,), (1,)))[:1] + 1e-06)
        kk = mm(k, k, ((1,), (1,))) * kn_col * kn_row
        qk = mm(q, k, ((1,), (1,))) * qn_col * kn_row
        for half in range(2):
            h = 2 * pair + half
            pick = lane == base + h
            g_col = jnp.sum(jnp.where(pick, sum_ref[...], 0.0), axis=1, keepdims=True)
            rate_col = jnp.sum(jnp.where(pick, rate_ref[...], 0.0), axis=1, keepdims=True)
            g_row = sumt_ref[h : h + 1, :]
            rate_row = ratet_ref[h : h + 1, :]
            ratio = jnp.where(inclusive, jnp.exp(jnp.where(inclusive, g_col - g_row, 0.0)), 0.0)
            lowers.append(jnp.where(strict, rate_col * ratio * kk, 0.0))
            heads.append((h, q, k, qf, kf, kn_col, qn_col, kn_row, g_col, g_row, rate_row, qk * ratio))
    inverses = unit_lower_inverses(lowers)
    for inverse, (h, q, k, qf, kf, kn_col, qn_col, kn_row, g_col, g_row, rate_row, scores) in zip(inverses, heads):
        mix = inverse * rate_row
        emat = mm(mix * (jnp.exp(g_row) * kn_row), k)
        last = g_col[n - 1 : n, :]
        ktail = kf * (kn_col * jnp.exp(last - g_col))
        a_ref[h] = (jnp.exp(last) * eye - mm(ktail, emat, ((0,), (0,)))).astype(BF)
        mbo_ref[h, :n, :] = mm(scores, mix).astype(BF)
        mbo_ref[h, n:, :] = mm(ktail, mix, ((0,), (0,))).astype(BF)
        g_ref[h] = (jnp.exp(g_col) * qn_col * qf - mm(scores, emat)).astype(BF)


def prepare(queries, keys, summed, rate):
    n = queries.shape[0]
    pairs = 4
    steps = HK // pairs
    heads = 2 * pairs
    return pl.pallas_call(
        lambda *refs: prepare_kernel(*refs, pairs=pairs),
        grid=(steps,),
        in_specs=[
            pl.BlockSpec((n, pairs * DK), lambda i: (0, i)),
            pl.BlockSpec((n, pairs * DK), lambda i: (0, i)),
            pl.BlockSpec((n, HV), lambda i: (0, 0)),
            pl.BlockSpec((n, HV), lambda i: (0, 0)),
            pl.BlockSpec((heads, n), lambda i: (i, 0)),
            pl.BlockSpec((heads, n), lambda i: (i, 0)),
        ],
        out_specs=[
            pl.BlockSpec((heads, 2 * n, n), lambda i: (i, 0, 0)),
            pl.BlockSpec((heads, DK, DK), lambda i: (i, 0, 0)),
            pl.BlockSpec((heads, n, DK), lambda i: (i, 0, 0)),
        ],
        out_shape=[
            jax.ShapeDtypeStruct((HV, 2 * n, n), BF),
            jax.ShapeDtypeStruct((HV, DK, DK), BF),
            jax.ShapeDtypeStruct((HV, n, DK), BF),
        ],
        cost_estimate=pl.CostEstimate(flops=4_000_000_000, bytes_accessed=4_000_000, transcendentals=0),
        name="prepare",
    )(queries, keys, summed, rate, summed.T, rate.T)


def reach_kernel(g_ref, a1_ref, a2_ref, out_ref):
    for h in range(g_ref.shape[0]):
        g = g_ref[h]
        g2 = mm(g, a1_ref[h]).astype(BF)
        out_ref[h, :, :DK] = g
        out_ref[h, :, DK : 2 * DK] = g2
        out_ref[h, :, 2 * DK :] = mm(g2, a2_ref[h]).astype(BF)


def reach(gmat, a1, a2):
    heads, n, _ = gmat.shape
    return pl.pallas_call(
        reach_kernel,
        out_shape=jax.ShapeDtypeStruct((heads, n, 3 * DK), BF),
        cost_estimate=pl.CostEstimate(flops=200_000_000, bytes_accessed=4_000_000, transcendentals=0),
        name="reach",
    )(gmat, a1, a2)


def values_kernel(moe_ref, res_ref, gain_ref, w_ref, mbo_ref, zero_ref, b_ref, normed):
    n = res_ref.shape[0]

    @pl.when(pl.program_id(0) == 0)
    def _():
        stream = (res_ref[...].astype(F32) + moe_ref[...].astype(F32)).astype(BF).astype(F32)
        scale = lax.rsqrt(jnp.mean(stream * stream, axis=-1, keepdims=True) + 1e-06)
        normed[...] = (stream * scale * gain_ref[...].astype(F32)).astype(BF)

    values = mm(normed[...], w_ref[...]).astype(BF)
    for h in range(mbo_ref.shape[0]):
        both = mm(mbo_ref[h], values[:, h * DV : (h + 1) * DV])
        zero_ref[:, h * DV : (h + 1) * DV] = both[:n]
        b_ref[h] = both[n:].astype(BF)


def project(moe, residual, gain, weight, mbo):
    n, width = residual.shape
    heads = 4
    return pl.pallas_call(
        values_kernel,
        grid=(HV // heads,),
        in_specs=[
            pl.BlockSpec((n, width), lambda i: (0, 0)),
            pl.BlockSpec((n, width), lambda i: (0, 0)),
            pl.BlockSpec((1, width), lambda i: (0, 0)),
            pl.BlockSpec((width, heads * DV), lambda i: (0, i)),
            pl.BlockSpec((heads, 2 * n, n), lambda i: (i, 0, 0)),
        ],
        out_specs=[
            pl.BlockSpec((n, heads * DV), lambda i: (0, i)),
            pl.BlockSpec((heads, DK, DV), lambda i: (i, 0, 0)),
        ],
        out_shape=[
            jax.ShapeDtypeStruct((n, HV * DV), F32),
            jax.ShapeDtypeStruct((HV, DK, DV), BF),
        ],
        scratch_shapes=[pltpu.VMEM((n, width), BF)],
        cost_estimate=pl.CostEstimate(flops=1_200_000_000, bytes_accessed=12_000_000, transcendentals=0),
        name="project",
    )(moe, residual, gain.reshape(1, width), weight, mbo)


def finish_kernel(zero_ref, reach_ref, b1_ref, b2_ref, b3_ref, out_ref):
    for h in range(reach_ref.shape[0]):
        total = zero_ref[:, h * DV : (h + 1) * DV]
        for d, b_ref in enumerate((b1_ref, b2_ref, b3_ref)):
            total += mm(reach_ref[h, :, d * DK : (d + 1) * DK], b_ref[h])
        out_ref[:, h * DV : (h + 1) * DV] = total.astype(BF)


def finish(zero, reached, b1, b2, b3):
    n = zero.shape[0]
    return pl.pallas_call(
        finish_kernel,
        out_shape=jax.ShapeDtypeStruct((n, HV * DV), BF),
        name="finish",
    )(zero, reached, b1, b2, b3)


def on_device(
    shape_x,
    expert_hidden,
    down_weight,
    residual,
    expert_ids,
    combine_weight,
    norm_gain,
    value_weight,
    queries,
    keys,
    log_decay,
    write_rate,
):
    n_ea = lax.axis_size("ea")
    n_sa = lax.axis_size("sa")
    exp_dev, ff_units, width = down_weight.shape
    cap = expert_hidden.shape[1] // n_ea
    experts = exp_dev * n_ea
    tokens = residual.shape[1]
    top = expert_ids.shape[2]
    plane = shape_x
    layers = n_ea // plane
    in_plane = [[z * plane + i for i in range(plane)] for z in range(layers)]
    across = [[z * plane + i for z in range(layers)] for i in range(plane)]
    me = lax.axis_index("ea")
    my_layer = me // plane

    hidden = expert_hidden.reshape(exp_dev, layers, plane, cap, ff_units).transpose(2, 0, 1, 3, 4)
    hidden = hidden.reshape(plane, exp_dev, layers * cap, ff_units)
    produced = jnp.einsum("perf,efd->perd", hidden, down_weight, preferred_element_type=F32).astype(BF)
    received = lax.all_to_all(
        produced, "ea", split_axis=0, concat_axis=0, tiled=True, axis_index_groups=in_plane
    )
    per_layer = plane * exp_dev * layers * cap
    received = received.reshape(per_layer, width)

    ids = expert_ids[0]
    onehot = ids[:, :, None] == jnp.arange(experts, dtype=jnp.int32)[None, None, :]
    counts = jnp.sum(onehot.astype(F32), axis=1)
    earlier = lax.broadcasted_iota(jnp.int32, (tokens, tokens), 0) > lax.broadcasted_iota(
        jnp.int32, (tokens, tokens), 1
    )
    prior = mm(earlier, counts)
    slots = jnp.sum(jnp.where(onehot, prior[:, None, :], 0.0), axis=-1)
    place = (ids // exp_dev) * (exp_dev * layers * cap) + (ids % exp_dev) * (layers * cap)
    route = jnp.concatenate([place.astype(F32) + slots, combine_weight[0]], axis=1)
    routes = lax.all_gather(route, "ea", axis=0, axis_index_groups=across)
    offset = (jnp.arange(layers) * cap - my_layer * per_layer).astype(F32)[:, None, None]
    where_to = (routes[:, :, :top] + offset).reshape(layers * tokens, top).astype(jnp.int32)
    amount = routes[:, :, top:].reshape(layers * tokens, top)
    slot_of = lax.broadcasted_iota(jnp.int32, (layers * tokens, per_layer), 1)
    mixing = jnp.zeros((layers * tokens, per_layer), F32)
    for i in range(top):
        mixing = mixing + jnp.where(slot_of == where_to[:, i : i + 1], amount[:, i : i + 1], 0.0)
    partial = mm(mixing, received).astype(BF)
    moe = lax.psum_scatter(
        partial.reshape(layers, tokens, width),
        "ea",
        scatter_dimension=0,
        axis_index_groups=across,
        tiled=False,
    )

    summed = jnp.cumsum(log_decay[0], axis=0)
    mbo, amat, gmat = prepare(queries[0], keys[0], summed, write_rate[0])

    def shifted(field, by):
        return lax.ppermute(field, "sa", [(i, i + by) for i in range(n_sa - by)])

    reached = reach(gmat, shifted(amat, 1), shifted(amat, 2))
    full_weight = lax.all_gather(value_weight, "ea", axis=0, tiled=True)
    zero, bmat = project(moe, residual[0], norm_gain, full_weight, mbo)
    out = finish(zero, reached, shifted(bmat, 1), shifted(bmat, 2), shifted(bmat, 3))
    return out[None]


def solution(mesh):
    def body(*args):
        return on_device(8, *args)

    return jax.shard_map(
        body,
        mesh=mesh,
        in_specs=(
            P("ea", "sa", None),
            P("ea", None, None),
            P("ea", "sa", None),
            P("ea", "sa", None),
            P("ea", "sa", None),
            P(),
            P("ea", None),
            P("ea", "sa", None),
            P("ea", "sa", None),
            P("ea", "sa", None),
            P("ea", "sa", None),
        ),
        out_specs=P("ea", "sa", None),
        check_vma=False,
    )
```

```python
import functools

import jax
import jax.numpy as jnp
import numpy as np
from jax import lax
from jax.experimental import pallas as pl
from jax.experimental.pallas import tpu as pltpu
from jax.sharding import PartitionSpec as P

HV = 16
HK = 8
DK = 128
DV = 128
BF = jnp.bfloat16
F32 = jnp.float32
MESH = pl.DeviceIdType.MESH


def mm(a, b, dims=((1,), (0,))):
    return lax.dot_general(a.astype(BF), b.astype(BF), (dims, ((), ())), preferred_element_type=F32)


def mm_full(a, b, dims=((1,), (0,))):
    return lax.dot_general(
        a, b, (dims, ((), ())), preferred_element_type=F32, precision=lax.Precision.HIGHEST
    )


def mm3(a, b):
    ah, bh = a.astype(BF), b.astype(BF)
    al = (a - ah.astype(F32)).astype(BF)
    bl = (b - bh.astype(F32)).astype(BF)
    return mm(ah, bh) + (mm(ah, bl) + mm(al, bh))


def unit_lower_inverses(lowers):
    n = lowers[0].shape[0]
    row = lax.broadcasted_iota(jnp.int32, (n, n), 0)
    col = lax.broadcasted_iota(jnp.int32, (n, n), 1)
    eye = (row == col).astype(F32)
    size = 16
    same = (row // size) == (col // size)
    powers = [jnp.where(same, -low, 0.0) for low in lowers]
    outs = [eye + p for p in powers]
    for _ in range(3):
        powers = [mm3(p, p) for p in powers]
        outs = [o + mm3(p, o) for p, o in zip(powers, outs)]
    while size < n:
        join = ((row // (2 * size)) == (col // (2 * size))) & ((row // size) > (col // size))
        parts = [mm3(jnp.where(join, low, 0.0), o) for low, o in zip(lowers, outs)]
        outs = [o - mm3(o, p) for o, p in zip(outs, parts)]
        size *= 2
    return outs


def prepare_kernel(q_ref, k_ref, sum_ref, rate_ref, sumt_ref, ratet_ref, mbo_ref, a_ref, g_ref, *, pairs):
    n = q_ref.shape[0]
    row = lax.broadcasted_iota(jnp.int32, (n, n), 0)
    col = lax.broadcasted_iota(jnp.int32, (n, n), 1)
    inclusive = row >= col
    strict = row > col
    eye = (row == col).astype(F32)
    ones = jnp.ones((8, DK), F32)
    base = pl.program_id(0) * (2 * pairs)
    lane = lax.broadcasted_iota(jnp.int32, (n, HV), 1)
    heads, lowers = [], []
    for pair in range(pairs):
        q = q_ref[:, pair * DK : (pair + 1) * DK]
        k = k_ref[:, pair * DK : (pair + 1) * DK]
        qf, kf = q.astype(F32), k.astype(F32)
        kn_col = lax.rsqrt(jnp.sum(kf * kf, axis=-1, keepdims=True) + 1e-06)
        qn_col = lax.rsqrt(jnp.sum(qf * qf, axis=-1, keepdims=True) + 1e-06) * DK ** (-0.5)
        kn_row = lax.rsqrt(mm_full(ones, kf * kf, ((1,), (1,)))[:1] + 1e-06)
        kk = mm(k, k, ((1,), (1,))) * kn_col * kn_row
        qk = mm(q, k, ((1,), (1,))) * qn_col * kn_row
        for half in range(2):
            h = 2 * pair + half
            pick = lane == base + h
            g_col = jnp.sum(jnp.where(pick, sum_ref[...], 0.0), axis=1, keepdims=True)
            rate_col = jnp.sum(jnp.where(pick, rate_ref[...], 0.0), axis=1, keepdims=True)
            g_row = sumt_ref[h : h + 1, :]
            rate_row = ratet_ref[h : h + 1, :]
            ratio = jnp.where(inclusive, jnp.exp(jnp.where(inclusive, g_col - g_row, 0.0)), 0.0)
            lowers.append(jnp.where(strict, rate_col * ratio * kk, 0.0))
            heads.append((h, q, k, qf, kf, kn_col, qn_col, kn_row, g_col, g_row, rate_row, qk * ratio))
    inverses = unit_lower_inverses(lowers)
    for inverse, (h, q, k, qf, kf, kn_col, qn_col, kn_row, g_col, g_row, rate_row, scores) in zip(inverses, heads):
        mix = inverse * rate_row
        emat = mm(mix * (jnp.exp(g_row) * kn_row), k)
        last = g_col[n - 1 : n, :]
        ktail = kf * (kn_col * jnp.exp(last - g_col))
        a_ref[h] = (jnp.exp(last) * eye - mm(ktail, emat, ((0,), (0,)))).astype(BF)
        for at, part in ((0, mm3(scores, mix)), (n, mm3(jnp.transpose(ktail), mix))):
            high = part.astype(BF)
            mbo_ref[h, at : at + n, :] = high
            mbo_ref[h, 2 * n + at : 3 * n + at, :] = (part - high.astype(F32)).astype(BF)
        g_ref[h] = (jnp.exp(g_col) * qn_col * qf - mm(scores, emat)).astype(BF)


def prepare(queries, keys, summed, rate):
    n = queries.shape[0]
    pairs = 4
    steps = HK // pairs
    heads = 2 * pairs
    return pl.pallas_call(
        lambda *refs: prepare_kernel(*refs, pairs=pairs),
        grid=(steps,),
        in_specs=[
            pl.BlockSpec((n, pairs * DK), lambda i: (0, i)),
            pl.BlockSpec((n, pairs * DK), lambda i: (0, i)),
            pl.BlockSpec((n, HV), lambda i: (0, 0)),
            pl.BlockSpec((n, HV), lambda i: (0, 0)),
            pl.BlockSpec((heads, n), lambda i: (i, 0)),
            pl.BlockSpec((heads, n), lambda i: (i, 0)),
        ],
        out_specs=[
            pl.BlockSpec((heads, 4 * n, n), lambda i: (i, 0, 0)),
            pl.BlockSpec((heads, DK, DK), lambda i: (i, 0, 0)),
            pl.BlockSpec((heads, n, DK), lambda i: (i, 0, 0)),
        ],
        out_shape=[
            jax.ShapeDtypeStruct((HV, 4 * n, n), BF),
            jax.ShapeDtypeStruct((HV, DK, DK), BF),
            jax.ShapeDtypeStruct((HV, n, DK), BF),
        ],
        cost_estimate=pl.CostEstimate(flops=4_000_000_000, bytes_accessed=4_000_000, transcendentals=0),
        name="prepare",
    )(queries, keys, summed, rate, summed.T, rate.T)


def reach_kernel(g_ref, a1_ref, a2_ref, out_ref):
    for h in range(g_ref.shape[0]):
        g = g_ref[h]
        g2 = mm(g, a1_ref[h]).astype(BF)
        out_ref[h, :, :DK] = g
        out_ref[h, :, DK : 2 * DK] = g2
        out_ref[h, :, 2 * DK :] = mm(g2, a2_ref[h]).astype(BF)


def reach(gmat, a1, a2):
    heads, n, _ = gmat.shape
    return pl.pallas_call(
        reach_kernel,
        out_shape=jax.ShapeDtypeStruct((heads, n, 3 * DK), BF),
        cost_estimate=pl.CostEstimate(flops=200_000_000, bytes_accessed=4_000_000, transcendentals=0),
        name="reach",
    )(gmat, a1, a2)


def values_kernel(moe_ref, res_ref, gain_ref, w_ref, mbo_ref, zero_ref, b_ref, normed):
    n = res_ref.shape[0]

    @pl.when(pl.program_id(0) == 0)
    def _():
        stream = (res_ref[...].astype(F32) + moe_ref[...].astype(F32)).astype(BF).astype(F32)
        scale = lax.rsqrt(jnp.mean(stream * stream, axis=-1, keepdims=True) + 1e-06)
        normed[...] = (stream * scale * gain_ref[...].astype(F32)).astype(BF)

    values = mm(normed[...], w_ref[0]).astype(BF)
    for h in range(mbo_ref.shape[0]):
        both = mm(mbo_ref[h], values[:, h * DV : (h + 1) * DV])
        both = both[: 2 * n] + both[2 * n :]
        zero_ref[:, h * DV : (h + 1) * DV] = both[:n]
        b_ref[h] = both[n:].astype(BF)


def project(moe, residual, gain, weight, mbo):
    n, width = residual.shape
    heads = 4
    return pl.pallas_call(
        values_kernel,
        grid=(HV // heads,),
        in_specs=[
            pl.BlockSpec((n, width), lambda i: (0, 0)),
            pl.BlockSpec((n, width), lambda i: (0, 0)),
            pl.BlockSpec((1, width), lambda i: (0, 0)),
            pl.BlockSpec((1, width, heads * DV), lambda i: (i, 0, 0)),
            pl.BlockSpec((heads, 4 * n, n), lambda i: (i, 0, 0)),
        ],
        out_specs=[
            pl.BlockSpec((n, heads * DV), lambda i: (0, i)),
            pl.BlockSpec((heads, DK, DV), lambda i: (i, 0, 0)),
        ],
        out_shape=[
            jax.ShapeDtypeStruct((n, HV * DV), F32),
            jax.ShapeDtypeStruct((HV, DK, DV), BF),
        ],
        scratch_shapes=[pltpu.VMEM((n, width), BF)],
        cost_estimate=pl.CostEstimate(flops=1_200_000_000, bytes_accessed=12_000_000, transcendentals=0),
        name="project",
    )(moe, residual, gain.reshape(1, width), weight, mbo)


def finish_kernel(zero_ref, reach_ref, b1_ref, b2_ref, b3_ref, out_ref):
    for h in range(reach_ref.shape[0]):
        total = zero_ref[:, h * DV : (h + 1) * DV]
        for d, b_ref in enumerate((b1_ref, b2_ref, b3_ref)):
            total += mm(reach_ref[h, :, d * DK : (d + 1) * DK], b_ref[h])
        out_ref[:, h * DV : (h + 1) * DV] = total.astype(BF)


def finish(zero, reached, b1, b2, b3):
    n = zero.shape[0]
    return pl.pallas_call(
        finish_kernel,
        out_shape=jax.ShapeDtypeStruct((n, HV * DV), BF),
        name="finish",
    )(zero, reached, b1, b2, b3)


def exchange_kernel(
    plane, layers, hid_ref, down_ref, order_ref, ids_ref, amount_ref, moe_ref,
    hidden, outgoing, incoming, mixing, dense, zout, zin, routes,
    xs, xr, zs, zr, rs, rr,
):
    exp_dev, rows, _ = hid_ref.shape
    tokens, top = ids_ref.shape
    chunks, _, block, wide = outgoing.shape
    cap = rows // (plane * layers)
    group = layers * cap
    per_layer = plane * block
    me = lax.axis_index("ea")
    spot, layer = me % plane, me // plane
    sign = 1 - 2 * (me % 2)
    half = layers // 2

    def device(z, p):
        return {"ea": ((z + 2 * layers) % layers) * plane + p % plane}

    barrier = pltpu.get_barrier_semaphore()
    for r in range(1, plane):
        pl.semaphore_signal(barrier, inc=1, device_id=device(layer, spot + r), device_id_type=MESH)
    for r in range(1, layers):
        pl.semaphore_signal(barrier, inc=1, device_id=device(layer + r, spot), device_id_type=MESH)
    pl.semaphore_wait(barrier, plane + layers - 2)

    experts = exp_dev * plane * layers
    lane = lax.broadcasted_iota(jnp.int32, (tokens, experts), 1)
    ids = ids_ref[...]
    counts = jnp.zeros((tokens, experts), F32)
    for i in range(top):
        counts += jnp.where(lane == ids[:, i : i + 1], 1.0, 0.0)
    trow = lax.broadcasted_iota(jnp.int32, (tokens, tokens), 0)
    tcol = lax.broadcasted_iota(jnp.int32, (tokens, tokens), 1)
    prior = mm(jnp.where(trow > tcol, 1.0, 0.0), counts)
    place = (ids // exp_dev) * block + (ids % exp_dev) * group
    columns = []
    for i in range(top):
        slot = jnp.sum(jnp.where(lane == ids[:, i : i + 1], prior, 0.0), axis=1, keepdims=True)
        columns.append(place[:, i : i + 1].astype(F32) + slot)
    columns += [amount_ref[:, i : i + 1] for i in range(top)]
    table = jnp.zeros((tokens, 128), F32)
    tl = lax.broadcasted_iota(jnp.int32, (tokens, 128), 1)
    for i, column in enumerate(columns):
        table = jnp.where(tl == i, column, table)
    deep = routes.shape[1]
    routes[layer] = jnp.transpose(table)[:deep]

    for e in range(exp_dev):
        hidden[e] = mm(order_ref[...], hid_ref[e]).astype(BF)

    def route_copy(r):
        return pltpu.make_async_remote_copy(
            src_ref=routes.at[layer],
            dst_ref=routes.at[layer],
            send_sem=rs.at[r],
            recv_sem=rr.at[r],
            device_id=device(layer + r, spot),
            device_id_type=MESH,
        )

    for r in range(1, layers):
        route_copy(r).start()

    def produce(c):
        at = pl.ds(pl.multiple_of(c * wide, wide), wide)
        made = [mm(hidden[e], down_ref[e, :, at]) for e in range(exp_dev)]
        for p in range(plane):
            mine = [m[p * group : (p + 1) * group] for m in made]
            outgoing[c, p] = jnp.concatenate(mine, axis=0).astype(BF)

    def ship(c):
        for r in range(1, plane):
            to = (spot + r) % plane
            pltpu.make_async_remote_copy(
                src_ref=outgoing.at[c, to],
                dst_ref=incoming.at[c, spot],
                send_sem=xs.at[c, r],
                recv_sem=xr.at[c, r],
                device_id=device(layer, to),
                device_id_type=MESH,
            ).start()
        incoming[c, spot] = outgoing[c, spot]

    produce(0)

    @pl.loop(1, chunks)
    def _(c):
        produce(c)
        ship(c - 1)

    ship(chunks - 1)

    for r in range(1, layers):
        route_copy(r).wait_recv()

    @pl.loop(0, layers)
    def _(z):
        table = jnp.concatenate([routes[z], jnp.zeros((128 - deep, tokens), F32)], axis=0)
        table = jnp.transpose(table)
        shift = (z * cap - layer * per_layer).astype(F32)
        start = pl.ds(pl.multiple_of(z * tokens, tokens), tokens)
        for k in range(per_layer // 256):
            slot_of = (lax.broadcasted_iota(jnp.int32, (tokens, 256), 1) + k * 256).astype(F32)
            total = jnp.zeros((tokens, 256), F32)
            for i in range(top):
                total += jnp.where(
                    slot_of == table[:, i : i + 1] + shift, table[:, top + i : top + i + 1], 0.0
                )
            mixing[start, k * 256 : (k + 1) * 256] = total.astype(BF)

    def hop(j, s):
        ahead = s < half
        step = s if ahead else s - half
        way = sign if ahead else -sign
        return pltpu.make_async_remote_copy(
            src_ref=zout.at[j, s],
            dst_ref=zin.at[j, s],
            send_sem=zs.at[j, s],
            recv_sem=zr.at[j, s],
            device_id=device(layer + way, spot),
            device_id_type=MESH,
        )

    def target(s):
        if s < half:
            return (layer + sign * (half - s) + 2 * layers) % layers
        return (layer - sign * (half - 1 - (s - half)) + 2 * layers) % layers

    hops = layers - 1

    def stage(j, s):
        sent = []
        for h in (s, s + half):
            if (h < half) == (h == s) and h < hops:
                part = dense[j % 5, target(h)]
                if s > 0:
                    hop(j, h - 1).wait_recv()
                    part = part + zin[j, h - 1].astype(F32)
                zout[j, h] = part.astype(BF)
                sent.append(h)
        for h in sent:
            hop(j, h).start()

    @pl.loop(0, chunks + half)
    def _(i):
        @pl.when(i >= half)
        def _():
            j = i - half
            hop(j, half - 1).wait_recv()
            hop(j, hops - 1).wait_recv()
            total = dense[j % 5, layer] + zin[j, half - 1].astype(F32) + zin[j, hops - 1].astype(F32)
            moe_ref[:, pl.ds(pl.multiple_of(j * wide, wide), wide)] = total

        for s in range(half - 1, 0, -1):
            @pl.when((i >= s) & (i < chunks + s))
            def _():
                stage(i - s, s)

        @pl.when(i < chunks)
        def _():
            for r in range(1, plane):
                pltpu.make_async_remote_copy(
                    src_ref=outgoing.at[i, spot],
                    dst_ref=incoming.at[i, spot],
                    send_sem=xs.at[i, r],
                    recv_sem=xr.at[i, r],
                    device_id=device(layer, spot + r),
                    device_id_type=MESH,
                ).wait_recv()
            rowsin = incoming[i].reshape(per_layer, wide)
            for z in range(layers):
                dense[i % 5, z] = mm(mixing[z * tokens : (z + 1) * tokens, :], rowsin)
            stage(i, 0)

    for r in range(1, layers):
        route_copy(r).wait_send()

    @pl.loop(0, chunks)
    def _(c):
        for r in range(1, plane):
            pltpu.make_async_remote_copy(
                src_ref=outgoing.at[c, spot],
                dst_ref=incoming.at[c, spot],
                send_sem=xs.at[c, r],
                recv_sem=xr.at[c, r],
                device_id=device(layer, spot + r),
                device_id_type=MESH,
            ).wait_send()
        for s in range(hops):
            hop(c, s).wait_send()


def exchange(plane, expert_hidden, down_weight, ids, amount):
    exp_dev, rows, ff_units = expert_hidden.shape
    width = down_weight.shape[2]
    n_ea = lax.axis_size("ea")
    layers = n_ea // plane
    cap = rows // n_ea
    tokens, top = ids.shape
    wide = 256
    chunks = width // wide
    block = exp_dev * layers * cap
    source = np.arange(rows).reshape(layers, plane, cap).transpose(1, 0, 2).reshape(-1)
    order = np.zeros((rows, rows), np.float32)
    order[np.arange(rows), source] = 1.0
    vmem = pl.BlockSpec(memory_space=pltpu.VMEM)
    dma = pltpu.SemaphoreType.DMA
    return pl.pallas_call(
        functools.partial(exchange_kernel, plane, layers),
        out_shape=jax.ShapeDtypeStruct((tokens, width), F32),
        in_specs=[vmem] * 5,
        out_specs=vmem,
        scratch_shapes=[
            pltpu.VMEM((exp_dev, rows, ff_units), BF),
            pltpu.VMEM((chunks, plane, block, wide), BF),
            pltpu.VMEM((chunks, plane, block, wide), BF),
            pltpu.VMEM((layers * tokens, plane * block), BF),
            pltpu.VMEM((5, layers, tokens, wide), F32),
            pltpu.VMEM((chunks, layers - 1, tokens, wide), BF),
            pltpu.VMEM((chunks, layers - 1, tokens, wide), BF),
            pltpu.VMEM((layers, 24, tokens), F32),
            dma((chunks, plane)),
            dma((chunks, plane)),
            dma((chunks, layers - 1)),
            dma((chunks, layers - 1)),
            dma((layers,)),
            dma((layers,)),
        ],
        compiler_params=pltpu.CompilerParams(
            collective_id=0, has_side_effects=True, vmem_limit_bytes=60 * 1024 * 1024
        ),
        cost_estimate=pl.CostEstimate(flops=60_000_000_000, bytes_accessed=12_000_000, transcendentals=0),
        name="exchange",
    )(expert_hidden, down_weight, jnp.asarray(order, BF), ids, amount)


def on_device(
    plane,
    expert_hidden,
    down_weight,
    residual,
    expert_ids,
    combine_weight,
    norm_gain,
    value_weight,
    queries,
    keys,
    log_decay,
    write_rate,
):
    n_sa = lax.axis_size("sa")
    moe = exchange(plane, expert_hidden, down_weight, expert_ids[0], combine_weight[0])

    summed = jnp.cumsum(log_decay[0], axis=0)
    mbo, amat, gmat = prepare(queries[0], keys[0], summed, write_rate[0])

    def shifted(field, by):
        return lax.ppermute(field, "sa", [(i, i + by) for i in range(n_sa - by)])

    reached = reach(gmat, shifted(amat, 1), shifted(amat, 2))
    share = value_weight.shape[1] // n_sa
    strip = lax.dynamic_slice_in_dim(value_weight, lax.axis_index("sa") * share, share, axis=1)
    strip = lax.all_gather(strip, "ea", axis=0, tiled=True)
    full_weight = lax.all_gather(strip, "sa", axis=0)
    zero, bmat = project(moe, residual[0], norm_gain, full_weight, mbo)
    out = finish(zero, reached, shifted(bmat, 1), shifted(bmat, 2), shifted(bmat, 3))
    return out[None]


def solution(mesh):
    def body(*args):
        return on_device(8, *args)

    return jax.shard_map(
        body,
        mesh=mesh,
        in_specs=(
            P("ea", "sa", None),
            P("ea", None, None),
            P("ea", "sa", None),
            P("ea", "sa", None),
            P("ea", "sa", None),
            P(),
            P("ea", None),
            P("ea", "sa", None),
            P("ea", "sa", None),
            P("ea", "sa", None),
            P("ea", "sa", None),
        ),
        out_specs=P("ea", "sa", None),
        check_vma=False,
    )
```

```python
import functools

import jax
import jax.numpy as jnp
import numpy as np
from jax import lax
from jax.experimental import pallas as pl
from jax.experimental.pallas import tpu as pltpu
from jax.sharding import PartitionSpec as P

HV = 16
HK = 8
DK = 128
DV = 128
BF = jnp.bfloat16
F32 = jnp.float32
MESH = pl.DeviceIdType.MESH


def mm(a, b, dims=((1,), (0,))):
    return lax.dot_general(a.astype(BF), b.astype(BF), (dims, ((), ())), preferred_element_type=F32)


def mm_full(a, b, dims=((1,), (0,))):
    return lax.dot_general(
        a, b, (dims, ((), ())), preferred_element_type=F32, precision=lax.Precision.HIGHEST
    )


def mm3(a, b):
    ah, bh = a.astype(BF), b.astype(BF)
    al = (a - ah.astype(F32)).astype(BF)
    bl = (b - bh.astype(F32)).astype(BF)
    return mm(ah, bh) + (mm(ah, bl) + mm(al, bh))


def unit_lower_inverses(lowers):
    n = lowers[0].shape[0]
    row = lax.broadcasted_iota(jnp.int32, (n, n), 0)
    col = lax.broadcasted_iota(jnp.int32, (n, n), 1)
    eye = (row == col).astype(F32)
    size = 16
    same = (row // size) == (col // size)
    powers = [jnp.where(same, -low, 0.0) for low in lowers]
    outs = [eye + p for p in powers]
    for _ in range(3):
        powers = [mm3(p, p) for p in powers]
        outs = [o + mm3(p, o) for p, o in zip(powers, outs)]
    while size < n:
        join = ((row // (2 * size)) == (col // (2 * size))) & ((row // size) > (col // size))
        parts = [mm3(jnp.where(join, low, 0.0), o) for low, o in zip(lowers, outs)]
        outs = [o - mm3(o, p) for o, p in zip(outs, parts)]
        size *= 2
    return outs


PAIRS = 4


def gates(decay_ref, rate_ref, gate):
    n, heads = decay_ref.shape
    row = lax.broadcasted_iota(jnp.int32, (n, n), 0)
    col = lax.broadcasted_iota(jnp.int32, (n, n), 1)
    blank = jnp.zeros((n, n - heads), F32)
    summed = mm_full(
        jnp.where(row >= col, 1.0, 0.0), jnp.concatenate([decay_ref[...], blank], axis=1)
    )
    gate[0] = summed
    gate[1] = jnp.transpose(summed)
    gate[2] = jnp.concatenate([rate_ref[...], blank], axis=1)
    gate[3] = jnp.transpose(jnp.concatenate([rate_ref[...], blank], axis=1))


def prepare_heads(step, q_ref, k_ref, gate, mbo_ref, a_ref, g_ref):
    pairs = PAIRS
    n = q_ref.shape[0]
    row = lax.broadcasted_iota(jnp.int32, (n, n), 0)
    col = lax.broadcasted_iota(jnp.int32, (n, n), 1)
    inclusive = row >= col
    strict = row > col
    eye = (row == col).astype(F32)
    ones = jnp.ones((8, DK), F32)
    base = step * (2 * pairs)
    heads, lowers = [], []
    wide = pl.ds(pl.multiple_of(step * (pairs * DK), pairs * DK), pairs * DK)
    all_q, all_k = q_ref[:, wide], k_ref[:, wide]
    these = pl.ds(pl.multiple_of(base, 2 * pairs), 2 * pairs)
    sum_rows, rate_rows = gate[1, these], gate[3, these]
    for pair in range(pairs):
        q = all_q[:, pair * DK : (pair + 1) * DK]
        k = all_k[:, pair * DK : (pair + 1) * DK]
        qf, kf = q.astype(F32), k.astype(F32)
        kn_col = lax.rsqrt(jnp.sum(kf * kf, axis=-1, keepdims=True) + 1e-06)
        qn_col = lax.rsqrt(jnp.sum(qf * qf, axis=-1, keepdims=True) + 1e-06) * DK ** (-0.5)
        kn_row = lax.rsqrt(mm_full(ones, kf * kf, ((1,), (1,)))[:1] + 1e-06)
        kk = mm(k, k, ((1,), (1,))) * kn_col * kn_row
        qk = mm(q, k, ((1,), (1,))) * qn_col * kn_row
        for half in range(2):
            h = 2 * pair + half
            pick = col == base + h
            g_col = jnp.sum(jnp.where(pick, gate[0], 0.0), axis=1, keepdims=True)
            rate_col = jnp.sum(jnp.where(pick, gate[2], 0.0), axis=1, keepdims=True)
            g_row = sum_rows[h : h + 1, :]
            rate_row = rate_rows[h : h + 1, :]
            ratio = jnp.where(inclusive, jnp.exp(jnp.where(inclusive, g_col - g_row, 0.0)), 0.0)
            lowers.append(jnp.where(strict, rate_col * ratio * kk, 0.0))
            heads.append((h, q, k, qf, kf, kn_col, qn_col, kn_row, g_col, g_row, rate_row, qk * ratio))
    inverses = unit_lower_inverses(lowers)
    for inverse, (h, q, k, qf, kf, kn_col, qn_col, kn_row, g_col, g_row, rate_row, scores) in zip(inverses, heads):
        mix = inverse * rate_row
        emat = mm(mix * (jnp.exp(g_row) * kn_row), k)
        last = g_col[n - 1 : n, :]
        ktail = kf * (kn_col * jnp.exp(last - g_col))
        a_ref[base + h] = (jnp.exp(last) * eye - mm(ktail, emat, ((0,), (0,)))).astype(BF)
        for at, part in ((0, mm3(scores, mix)), (n, mm3(jnp.transpose(ktail), mix))):
            high = part.astype(BF)
            mbo_ref[base + h, at : at + n, :] = high
            mbo_ref[base + h, 2 * n + at : 3 * n + at, :] = (part - high.astype(F32)).astype(BF)
        g_ref[base + h] = (jnp.exp(g_col) * qn_col * qf - mm(scores, emat)).astype(BF)


def layer_kernel(
    plane, layers, hid_ref, down_ref, order_ref, ids_ref, amount_ref, res_ref, gain_ref, value_ref,
    q_ref, k_ref, decay_ref, rate_ref, out_ref,
    hidden, down, outgoing, incoming, mixing, dense, zout, zin, routes, moe,
    weight, mbo, amat, gmat, gate, fresh, later, earlier,
    dsem, xs, xr, zs, zr, rs, rr, ws, wr, ss, sr,
):
    exp_dev, rows, _ = hid_ref.shape
    tokens, top = ids_ref.shape
    chunks, _, block, wide = outgoing.shape
    cap = rows // (plane * layers)
    group = layers * cap
    per_layer = plane * block
    me = lax.axis_index("ea")
    spot, layer = me % plane, me // plane
    sign = 1 - 2 * (me % 2)
    half = layers // 2

    y = lax.axis_index("sa")
    n_sa = lax.axis_size("sa")
    core = me % 2
    strip = y * 2 + core
    near = spot // 2

    def chunk_copy(c):
        at = pl.ds(pl.multiple_of(c * wide, wide), wide)
        return pltpu.make_async_copy(down_ref.at[:, :, at], down.at[c % depth], dsem.at[c % depth])

    depth = down.shape[0]
    for c in range(depth):
        chunk_copy(c).start()

    def device(z, p):
        return {"ea": ((z + 2 * layers) % layers) * plane + p % plane}

    barrier = pltpu.get_barrier_semaphore()
    for r in range(1, plane):
        pl.semaphore_signal(barrier, inc=1, device_id=device(layer, spot + r), device_id_type=MESH)
    for r in range(1, layers):
        pl.semaphore_signal(barrier, inc=1, device_id=device(layer + r, spot), device_id_type=MESH)
    for r in range(1, n_sa):
        pl.semaphore_signal(barrier, inc=1, device_id={"sa": (y + r) % n_sa}, device_id_type=MESH)
    pl.semaphore_wait(barrier, plane + layers + n_sa - 3)

    own_rows, part = value_ref.shape[0], weight.shape[2]

    def remote(src, dst, at, to):
        return pltpu.make_async_remote_copy(
            src_ref=src, dst_ref=dst, send_sem=ws.at[at], recv_sem=wr.at[at],
            device_id=to, device_id_type=MESH,
        )

    def weight_rows(start, size):
        return weight.at[strip, pl.ds(pl.multiple_of(start * size, size), size)]

    def copy_beside():
        other = y * 2 + 1 - core
        cols = pl.ds(pl.multiple_of(other * part, part), part)
        mine = pl.ds(pl.multiple_of(me * own_rows, own_rows), own_rows)
        return remote(value_ref.at[:, cols], weight.at[other, mine], 0, {"ea": me + 1 - 2 * core})

    def copy_x(r):
        ref = weight_rows(me // 2, 2 * own_rows)
        return remote(ref, ref, r, device(layer, ((near + r) % (plane // 2)) * 2 + core))

    def copy_z(r):
        ref = weight_rows(layer, plane * own_rows)
        return remote(ref, ref, 3 + r, device(layer + r, spot))

    def copy_y(r):
        return remote(weight.at[strip], weight.at[strip], 10 + r, {"sa": (y + r) % n_sa})

    def copy_last(q):
        ref = weight.at[((y + q) % n_sa) * 2 + core]
        return remote(ref, ref, 14 + (y + q) % n_sa, {"ea": me + 1 - 2 * core})

    def landed(q):
        ref = weight.at[((y + q) % n_sa) * 2 + 1 - core]
        return remote(ref, ref, 14 + (y + q) % n_sa, {"ea": me + 1 - 2 * core})

    copy_beside().start()
    weight[strip, pl.ds(pl.multiple_of(me * own_rows, own_rows), own_rows)] = value_ref[
        :, pl.ds(pl.multiple_of(strip * part, part), part)
    ]

    experts = exp_dev * plane * layers
    lane = lax.broadcasted_iota(jnp.int32, (tokens, experts), 1)
    ids = ids_ref[...]
    counts = jnp.zeros((tokens, experts), F32)
    for i in range(top):
        counts += jnp.where(lane == ids[:, i : i + 1], 1.0, 0.0)
    trow = lax.broadcasted_iota(jnp.int32, (tokens, tokens), 0)
    tcol = lax.broadcasted_iota(jnp.int32, (tokens, tokens), 1)
    prior = mm(jnp.where(trow > tcol, 1.0, 0.0), counts)
    place = (ids // exp_dev) * block + (ids % exp_dev) * group
    columns = []
    for i in range(top):
        slot = jnp.sum(jnp.where(lane == ids[:, i : i + 1], prior, 0.0), axis=1, keepdims=True)
        columns.append(place[:, i : i + 1].astype(F32) + slot)
    columns += [amount_ref[:, i : i + 1] for i in range(top)]
    table = jnp.zeros((tokens, 128), F32)
    tl = lax.broadcasted_iota(jnp.int32, (tokens, 128), 1)
    for i, column in enumerate(columns):
        table = jnp.where(tl == i, column, table)
    deep = routes.shape[1]
    routes[layer] = jnp.transpose(table)[:deep]

    for e in range(exp_dev):
        hidden[e] = mm(order_ref[...], hid_ref[e]).astype(BF)

    def route_copy(r):
        return pltpu.make_async_remote_copy(
            src_ref=routes.at[layer],
            dst_ref=routes.at[layer],
            send_sem=rs.at[r],
            recv_sem=rr.at[r],
            device_id=device(layer + r, spot),
            device_id_type=MESH,
        )

    for r in range(1, layers):
        route_copy(r).start()

    copy_beside().wait_recv()
    for r in range(1, plane // 2):
        copy_x(r).start()

    def produce(c):
        chunk_copy(c).wait()
        made = [mm(hidden[e], down[c % depth, e]) for e in range(exp_dev)]
        for p in range(plane):
            mine = [m[p * group : (p + 1) * group] for m in made]
            outgoing[c, p] = jnp.concatenate(mine, axis=0).astype(BF)

        @pl.when(c + depth < chunks)
        def _():
            chunk_copy(c + depth).start()

    def ship(c):
        for r in range(1, plane):
            to = (spot + r) % plane
            pltpu.make_async_remote_copy(
                src_ref=outgoing.at[c, to],
                dst_ref=incoming.at[c, spot],
                send_sem=xs.at[c, r],
                recv_sem=xr.at[c, r],
                device_id=device(layer, to),
                device_id_type=MESH,
            ).start()
        incoming[c, spot] = outgoing[c, spot]

    produce(0)

    @pl.loop(1, chunks)
    def _(c):
        produce(c)
        ship(c - 1)

    ship(chunks - 1)

    for r in range(1, plane // 2):
        copy_x(r).wait_recv()
    for r in range(1, layers):
        copy_z(r).start()
    for r in range(1, layers):
        route_copy(r).wait_recv()

    @pl.loop(0, layers)
    def _(z):
        table = jnp.concatenate([routes[z], jnp.zeros((128 - deep, tokens), F32)], axis=0)
        table = jnp.transpose(table)
        shift = (z * cap - layer * per_layer).astype(F32)
        start = pl.ds(pl.multiple_of(z * tokens, tokens), tokens)
        for k in range(per_layer // 256):
            slot_of = (lax.broadcasted_iota(jnp.int32, (tokens, 256), 1) + k * 256).astype(F32)
            total = jnp.zeros((tokens, 256), F32)
            for i in range(top):
                total += jnp.where(
                    slot_of == table[:, i : i + 1] + shift, table[:, top + i : top + i + 1], 0.0
                )
            mixing[start, k * 256 : (k + 1) * 256] = total.astype(BF)

    gates(decay_ref, rate_ref, gate)
    prepare_heads(0, q_ref, k_ref, gate, mbo, amat, gmat)
    for r in range(1, layers):
        copy_z(r).wait_recv()
    for r in range(1, n_sa):
        copy_y(r).start()
    copy_last(0).start()

    @pl.loop(1, HK // PAIRS)
    def _(step):
        prepare_heads(step, q_ref, k_ref, gate, mbo, amat, gmat)

    def hop(j, s):
        ahead = s < half
        step = s if ahead else s - half
        way = sign if ahead else -sign
        return pltpu.make_async_remote_copy(
            src_ref=zout.at[j, s],
            dst_ref=zin.at[j, s],
            send_sem=zs.at[j, s],
            recv_sem=zr.at[j, s],
            device_id=device(layer + way, spot),
            device_id_type=MESH,
        )

    def target(s):
        if s < half:
            return (layer + sign * (half - s) + 2 * layers) % layers
        return (layer - sign * (half - 1 - (s - half)) + 2 * layers) % layers

    hops = layers - 1

    def stage(j, s):
        sent = []
        for h in (s, s + half):
            if (h < half) == (h == s) and h < hops:
                part = dense[j % 5, target(h)]
                if s > 0:
                    hop(j, h - 1).wait_recv()
                    part = part + zin[j, h - 1].astype(F32)
                zout[j, h] = part.astype(BF)
                sent.append(h)
        for h in sent:
            hop(j, h).start()

    @pl.loop(0, chunks + half)
    def _(i):
        @pl.when(i >= half)
        def _():
            j = i - half
            hop(j, half - 1).wait_recv()
            hop(j, hops - 1).wait_recv()
            total = dense[j % 5, layer] + zin[j, half - 1].astype(F32) + zin[j, hops - 1].astype(F32)
            cols = pl.ds(pl.multiple_of(j * wide, wide), wide)
            moe[:, cols] = (res_ref[:, cols].astype(F32) + total).astype(BF)

        for s in range(half - 1, 0, -1):
            @pl.when((i >= s) & (i < chunks + s))
            def _():
                stage(i - s, s)

        @pl.when(i < chunks)
        def _():
            for r in range(1, plane):
                pltpu.make_async_remote_copy(
                    src_ref=outgoing.at[i, spot],
                    dst_ref=incoming.at[i, spot],
                    send_sem=xs.at[i, r],
                    recv_sem=xr.at[i, r],
                    device_id=device(layer, spot + r),
                    device_id_type=MESH,
                ).wait_recv()
            rowsin = incoming[i].reshape(per_layer, wide)
            for z in range(layers):
                dense[i % 5, z] = mm(mixing[z * tokens : (z + 1) * tokens, :], rowsin)
            stage(i, 0)

        @pl.when(i == chunks)
        def _():
            for r in range(1, n_sa):
                copy_y(r).wait_recv()
            for q in range(1, n_sa):
                copy_last(q).start()

    stream = moe[...].astype(F32)
    scale = lax.rsqrt(jnp.mean(stream * stream, axis=-1, keepdims=True) + 1e-06)
    moe[...] = (stream * scale * gain_ref[...].astype(F32)).astype(BF)
    for q in range(n_sa):
        landed(q).wait_recv()

    pair = part // DV

    def pass_on(b):
        return pltpu.make_async_remote_copy(
            src_ref=later.at[b], dst_ref=earlier.at[b], send_sem=ss.at[b], recv_sem=sr.at[b],
            device_id={"sa": (y + 1) % n_sa}, device_id_type=MESH,
        )

    strips = weight.shape[0]

    @pl.loop(0, strips)
    def _(b):
        values = mm(moe[...], weight[b]).astype(BF)
        for h in range(pair):
            both = mm(mbo[b * pair + h], values[:, h * DV : (h + 1) * DV])
            both = both[: 2 * tokens] + both[2 * tokens :]
            fresh[b * pair + h] = both

        @pl.when(y == 0)
        def _():
            for h in range(pair):
                later[b, h] = fresh[b * pair + h, tokens:].astype(BF)
            pass_on(b).start()

    @pl.loop(0, strips)
    def _(b):
        cols = pl.ds(pl.multiple_of(b * part, part), part)

        @pl.when(y == 0)
        def _():
            parts = [fresh[b * pair + h, :tokens] for h in range(pair)]
            out_ref[:, cols] = jnp.concatenate(parts, axis=1).astype(BF)

        @pl.when(y > 0)
        def _():
            pass_on(b).wait_recv()

            @pl.when(y < n_sa - 1)
            def _():
                for h in range(pair):
                    at = b * pair + h
                    later[b, h] = (mm(amat[at], earlier[b, h]) + fresh[at, tokens:]).astype(BF)
                pass_on(b).start()

            parts = [
                fresh[b * pair + h, :tokens] + mm(gmat[b * pair + h], earlier[b, h]) for h in range(pair)
            ]
            out_ref[:, cols] = jnp.concatenate(parts, axis=1).astype(BF)

    @pl.when(y < n_sa - 1)
    def _():
        for b in range(strips):
            pass_on(b).wait_send()

    copy_beside().wait_send()
    for r in range(1, plane // 2):
        copy_x(r).wait_send()
    for r in range(1, layers):
        copy_z(r).wait_send()
    for r in range(1, n_sa):
        copy_y(r).wait_send()
    for q in range(n_sa):
        copy_last(q).wait_send()
    for r in range(1, layers):
        route_copy(r).wait_send()

    @pl.loop(0, chunks)
    def _(c):
        for r in range(1, plane):
            pltpu.make_async_remote_copy(
                src_ref=outgoing.at[c, spot],
                dst_ref=incoming.at[c, spot],
                send_sem=xs.at[c, r],
                recv_sem=xr.at[c, r],
                device_id=device(layer, spot + r),
                device_id_type=MESH,
            ).wait_send()
        for s in range(hops):
            hop(c, s).wait_send()


def layer(
    plane, expert_hidden, down_weight, residual, ids, amount, gain, value_weight, queries, keys, decay, rate
):
    exp_dev, rows, ff_units = expert_hidden.shape
    width = down_weight.shape[2]
    n_ea = lax.axis_size("ea")
    n_sa = lax.axis_size("sa")
    layers = n_ea // plane
    cap = rows // n_ea
    tokens, top = ids.shape
    wide = 256
    chunks = width // wide
    block = exp_dev * layers * cap
    source = np.arange(rows).reshape(layers, plane, cap).transpose(1, 0, 2).reshape(-1)
    order = np.zeros((rows, rows), np.float32)
    order[np.arange(rows), source] = 1.0
    strips = 2 * n_sa
    part = width // strips
    vmem = pl.BlockSpec(memory_space=pltpu.VMEM)
    hbm = pl.BlockSpec(memory_space=pl.ANY)
    dma = pltpu.SemaphoreType.DMA
    return pl.pallas_call(
        functools.partial(layer_kernel, plane, layers),
        out_shape=jax.ShapeDtypeStruct((tokens, width), BF),
        in_specs=[vmem, hbm] + [vmem] * 10,
        out_specs=vmem,
        scratch_shapes=[
            pltpu.VMEM((exp_dev, rows, ff_units), BF),
            pltpu.VMEM((3, exp_dev, ff_units, wide), BF),
            pltpu.VMEM((chunks, plane, block, wide), BF),
            pltpu.VMEM((chunks, plane, block, wide), BF),
            pltpu.VMEM((layers * tokens, plane * block), BF),
            pltpu.VMEM((5, layers, tokens, wide), F32),
            pltpu.VMEM((chunks, layers - 1, tokens, wide), BF),
            pltpu.VMEM((chunks, layers - 1, tokens, wide), BF),
            pltpu.VMEM((layers, 24, tokens), F32),
            pltpu.VMEM((tokens, width), BF),
            pltpu.VMEM((strips, width, part), BF),
            pltpu.VMEM((HV, 4 * tokens, tokens), BF),
            pltpu.VMEM((HV, DK, DK), BF),
            pltpu.VMEM((HV, tokens, DK), BF),
            pltpu.VMEM((4, tokens, 128), F32),
            pltpu.VMEM((HV, tokens + DK, DV), F32),
            pltpu.VMEM((strips, part // DV, DK, DV), BF),
            pltpu.VMEM((strips, part // DV, DK, DV), BF),
            dma((3,)),
            dma((chunks, plane)),
            dma((chunks, plane)),
            dma((chunks, layers - 1)),
            dma((chunks, layers - 1)),
            dma((layers,)),
            dma((layers,)),
            dma((18,)),
            dma((18,)),
            dma((strips,)),
            dma((strips,)),
        ],
        compiler_params=pltpu.CompilerParams(
            collective_id=0, has_side_effects=True, vmem_limit_bytes=63 * 1024 * 1024
        ),
        cost_estimate=pl.CostEstimate(flops=60_000_000_000, bytes_accessed=12_000_000, transcendentals=0),
        name="layer",
    )(
        expert_hidden, down_weight, jnp.asarray(order, BF), ids, amount, residual,
        gain.reshape(1, width), value_weight, queries, keys, decay, rate,
    )


def solution(mesh):
    def body(
        expert_hidden, down_weight, residual, expert_ids, combine_weight, norm_gain, value_weight,
        queries, keys, log_decay, write_rate,
    ):
        return layer(
            8, expert_hidden, down_weight, residual[0], expert_ids[0], combine_weight[0], norm_gain,
            value_weight, queries[0], keys[0], log_decay[0], write_rate[0],
        )[None]

    return jax.shard_map(
        body,
        mesh=mesh,
        in_specs=(
            P("ea", "sa", None),
            P("ea", None, None),
            P("ea", "sa", None),
            P("ea", "sa", None),
            P("ea", "sa", None),
            P(),
            P("ea", None),
            P("ea", "sa", None),
            P("ea", "sa", None),
            P("ea", "sa", None),
            P("ea", "sa", None),
        ),
        out_specs=P("ea", "sa", None),
        check_vma=False,
    )
```

```python
import functools

import jax
import jax.numpy as jnp
import numpy as np
from jax import lax
from jax.experimental import pallas as pl
from jax.experimental.pallas import tpu as pltpu
from jax.sharding import PartitionSpec as P

HV = 16
HK = 8
DK = 128
DV = 128
BF = jnp.bfloat16
F32 = jnp.float32
MESH = pl.DeviceIdType.MESH


def mm(a, b, dims=((1,), (0,))):
    return lax.dot_general(a.astype(BF), b.astype(BF), (dims, ((), ())), preferred_element_type=F32)


def mm_full(a, b, dims=((1,), (0,))):
    return lax.dot_general(
        a, b, (dims, ((), ())), preferred_element_type=F32, precision=lax.Precision.HIGHEST
    )


def mm3(a, b):
    ah, bh = a.astype(BF), b.astype(BF)
    al = (a - ah.astype(F32)).astype(BF)
    bl = (b - bh.astype(F32)).astype(BF)
    return mm(ah, bh) + (mm(ah, bl) + mm(al, bh))


def unit_lower_inverses(lowers):
    n = lowers[0].shape[0]
    row = lax.broadcasted_iota(jnp.int32, (n, n), 0)
    col = lax.broadcasted_iota(jnp.int32, (n, n), 1)
    eye = (row == col).astype(F32)
    size = 16
    same = (row // size) == (col // size)
    powers = [jnp.where(same, -low, 0.0) for low in lowers]
    outs = [eye + p for p in powers]
    for _ in range(3):
        powers = [mm3(p, p) for p in powers]
        outs = [o + mm3(p, o) for p, o in zip(powers, outs)]
    while size < n:
        join = ((row // (2 * size)) == (col // (2 * size))) & ((row // size) > (col // size))
        parts = [mm3(jnp.where(join, low, 0.0), o) for low, o in zip(lowers, outs)]
        outs = [o - mm3(o, p) for o, p in zip(outs, parts)]
        size *= 2
    return outs


PAIRS = 4


def gates(decay_ref, rate_ref, gate):
    heads, n = decay_ref.shape
    row = lax.broadcasted_iota(jnp.int32, (n, n), 0)
    col = lax.broadcasted_iota(jnp.int32, (n, n), 1)
    blank = jnp.zeros((n - heads, n), F32)
    summed = mm_full(decay_ref[...], jnp.where(row <= col, 1.0, 0.0))
    for at, rows in ((0, summed), (2, rate_ref[...])):
        rows = jnp.concatenate([rows, blank], axis=0)
        gate[at] = jnp.transpose(rows)
        gate[at + 1] = rows


def prepare_heads(step, q_ref, k_ref, gate, mbo_ref, a_ref, g_ref):
    pairs = PAIRS
    n = q_ref.shape[0]
    row = lax.broadcasted_iota(jnp.int32, (n, n), 0)
    col = lax.broadcasted_iota(jnp.int32, (n, n), 1)
    inclusive = row >= col
    strict = row > col
    eye = (row == col).astype(F32)
    ones = jnp.ones((8, DK), F32)
    base = step * (2 * pairs)
    heads, lowers = [], []
    wide = pl.ds(pl.multiple_of(step * (pairs * DK), pairs * DK), pairs * DK)
    all_q, all_k = q_ref[:, wide], k_ref[:, wide]
    these = pl.ds(pl.multiple_of(base, 2 * pairs), 2 * pairs)
    sum_rows, rate_rows = gate[1, these], gate[3, these]
    for pair in range(pairs):
        q = all_q[:, pair * DK : (pair + 1) * DK]
        k = all_k[:, pair * DK : (pair + 1) * DK]
        qf, kf = q.astype(F32), k.astype(F32)
        kn_col = lax.rsqrt(jnp.sum(kf * kf, axis=-1, keepdims=True) + 1e-06)
        qn_col = lax.rsqrt(jnp.sum(qf * qf, axis=-1, keepdims=True) + 1e-06) * DK ** (-0.5)
        kn_row = lax.rsqrt(mm_full(ones, kf * kf, ((1,), (1,)))[:1] + 1e-06)
        kk = mm(k, k, ((1,), (1,))) * kn_col * kn_row
        qk = mm(q, k, ((1,), (1,))) * qn_col * kn_row
        for half in range(2):
            h = 2 * pair + half
            pick = col == base + h
            g_col = jnp.sum(jnp.where(pick, gate[0], 0.0), axis=1, keepdims=True)
            rate_col = jnp.sum(jnp.where(pick, gate[2], 0.0), axis=1, keepdims=True)
            g_row = sum_rows[h : h + 1, :]
            rate_row = rate_rows[h : h + 1, :]
            ratio = jnp.where(inclusive, jnp.exp(jnp.where(inclusive, g_col - g_row, 0.0)), 0.0)
            lowers.append(jnp.where(strict, rate_col * ratio * kk, 0.0))
            heads.append((h, q, k, qf, kf, kn_col, qn_col, kn_row, g_col, g_row, rate_row, qk * ratio))
    inverses = unit_lower_inverses(lowers)
    for inverse, (h, q, k, qf, kf, kn_col, qn_col, kn_row, g_col, g_row, rate_row, scores) in zip(inverses, heads):
        mix = inverse * rate_row
        emat = mm(mix * (jnp.exp(g_row) * kn_row), k)
        last = g_col[n - 1 : n, :]
        ktail = kf * (kn_col * jnp.exp(last - g_col))
        a_ref[base + h] = (jnp.exp(last) * eye - mm(ktail, emat, ((0,), (0,)))).astype(BF)
        for at, part in ((0, mm3(scores, mix)), (n, mm3(jnp.transpose(ktail), mix))):
            high = part.astype(BF)
            mbo_ref[base + h, at : at + n, :] = high
            mbo_ref[base + h, 2 * n + at : 3 * n + at, :] = (part - high.astype(F32)).astype(BF)
        g_ref[base + h] = (jnp.exp(g_col) * qn_col * qf - mm(scores, emat)).astype(BF)


def layer_kernel(
    plane, layers, hid_ref, down_ref, order_ref, ids_ref, amount_ref, res_ref, gain_ref, value_ref,
    q_ref, k_ref, decay_ref, rate_ref, out_ref,
    hidden, down, outgoing, incoming, mixing, dense, zout, zin, routes, moe,
    weight, mbo, amat, gmat, gate, fresh, later, earlier,
    dsem, xs, xr, zs, zr, rs, rr, ws, wr, ss, sr,
):
    exp_dev, rows, _ = hid_ref.shape
    top, _, tokens = ids_ref.shape
    _, chunks, block, wide = outgoing.shape
    full = chunks - 1
    units = chunks + 1

    def span(u):
        if isinstance(u, int) and u >= full:
            return full, (u - full) * (wide // 2), wide // 2
        return u, 0, wide
    cap = rows // (plane * layers)
    group = layers * cap
    per_layer = plane * block
    me = lax.axis_index("ea")
    spot, layer = me % plane, me // plane
    sign = 1 - 2 * (me % 2)
    half = layers // 2

    y = lax.axis_index("sa")
    n_sa = lax.axis_size("sa")
    core = me % 2
    strip = y * 2 + core
    near = spot // 2

    def chunk_copy(c):
        at = pl.ds(pl.multiple_of(c * wide, wide), wide)
        return pltpu.make_async_copy(down_ref.at[:, :, at], down.at[c % depth], dsem.at[c % depth])

    depth = down.shape[0]
    for c in range(depth):
        chunk_copy(c).start()

    def device(z, p):
        return {"ea": ((z + 2 * layers) % layers) * plane + p % plane}

    barrier = pltpu.get_barrier_semaphore()
    for r in range(1, plane):
        pl.semaphore_signal(barrier, inc=1, device_id=device(layer, spot + r), device_id_type=MESH)
    for r in range(1, layers):
        pl.semaphore_signal(barrier, inc=1, device_id=device(layer + r, spot), device_id_type=MESH)
    for r in range(1, n_sa):
        pl.semaphore_signal(barrier, inc=1, device_id={"sa": (y + r) % n_sa}, device_id_type=MESH)

    own_rows, part = value_ref.shape[0], weight.shape[2]

    def remote(src, dst, at, to):
        return pltpu.make_async_remote_copy(
            src_ref=src, dst_ref=dst, send_sem=ws.at[at], recv_sem=wr.at[at],
            device_id=to, device_id_type=MESH,
        )

    def weight_rows(start, size):
        return weight.at[strip, pl.ds(pl.multiple_of(start * size, size), size)]

    def copy_beside():
        other = y * 2 + 1 - core
        cols = pl.ds(pl.multiple_of(other * part, part), part)
        mine = pl.ds(pl.multiple_of(me * own_rows, own_rows), own_rows)
        return remote(value_ref.at[:, cols], weight.at[other, mine], 0, {"ea": me + 1 - 2 * core})

    def copy_x(r):
        ref = weight_rows(me // 2, 2 * own_rows)
        return remote(ref, ref, r, device(layer, ((near + r) % (plane // 2)) * 2 + core))

    def copy_z(r):
        ref = weight_rows(layer, plane * own_rows)
        return remote(ref, ref, 3 + r, device(layer + r, spot))

    def copy_y(r):
        return remote(weight.at[strip], weight.at[strip], 10 + r, {"sa": (y + r) % n_sa})

    def copy_last(q):
        ref = weight.at[((y + q) % n_sa) * 2 + core]
        return remote(ref, ref, 14 + (y + q) % n_sa, {"ea": me + 1 - 2 * core})

    def landed(q):
        ref = weight.at[((y + q) % n_sa) * 2 + 1 - core]
        return remote(ref, ref, 14 + (y + q) % n_sa, {"ea": me + 1 - 2 * core})

    weight[strip, pl.ds(pl.multiple_of(me * own_rows, own_rows), own_rows)] = value_ref[
        :, pl.ds(pl.multiple_of(strip * part, part), part)
    ]

    experts = exp_dev * plane * layers
    name = lax.broadcasted_iota(jnp.int32, (experts, tokens), 0)
    counts = jnp.zeros((experts, tokens), F32)
    for i in range(top):
        counts += jnp.where(name == ids_ref[i], 1.0, 0.0)
    trow = lax.broadcasted_iota(jnp.int32, (tokens, tokens), 0)
    tcol = lax.broadcasted_iota(jnp.int32, (tokens, tokens), 1)
    prior = mm(counts, jnp.where(trow < tcol, 1.0, 0.0))
    found = []
    for i in range(top):
        ids = ids_ref[i]
        slot = jnp.sum(jnp.where(name == ids, prior, 0.0), axis=0, keepdims=True)
        place = (ids // exp_dev) * block + (ids % exp_dev) * group
        found.append(place.astype(F32) + slot)
    found += [amount_ref[i] for i in range(top)]
    deep = routes.shape[1]
    found.append(jnp.zeros((deep - 2 * top, tokens), F32))
    routes[layer] = jnp.concatenate(found, axis=0)

    for e in range(exp_dev):
        hidden[e] = mm(order_ref[...], hid_ref[e]).astype(BF)

    def route_copy(r):
        return pltpu.make_async_remote_copy(
            src_ref=routes.at[layer],
            dst_ref=routes.at[layer],
            send_sem=rs.at[r],
            recv_sem=rr.at[r],
            device_id=device(layer + r, spot),
            device_id_type=MESH,
        )

    def produce(c):
        chunk_copy(c).wait()
        made = [mm(hidden[e], down[c % depth, e]) for e in range(exp_dev)]
        for p in range(plane):
            mine = [m[p * group : (p + 1) * group] for m in made]
            outgoing[p, c] = jnp.concatenate(mine, axis=0).astype(BF)

        @pl.when(c + depth < chunks)
        def _():
            chunk_copy(c + depth).start()

    def block_of(ref, p, u):
        c, at, size = span(u)
        return ref.at[p, c, :, pl.ds(at, size)]

    def ship(u):
        def send(to):
            pltpu.make_async_remote_copy(
                src_ref=block_of(outgoing, to, u),
                dst_ref=block_of(incoming, spot, u),
                send_sem=xs.at[u],
                recv_sem=xr.at[u],
                device_id=device(layer, to),
                device_id_type=MESH,
            ).start()

        for c in range(2):
            for dx in (2, 1, 3):
                send(((near + sign * dx + plane) % (plane // 2)) * 2 + c)
        send(spot + 1 - 2 * core)
        c, at, size = span(u)
        incoming[spot, c, :, at : at + size] = outgoing[spot, c, :, at : at + size]

    def shipped(u):
        return pltpu.make_async_remote_copy(
            src_ref=block_of(outgoing, pl.ds(0, plane - 1), u),
            dst_ref=block_of(incoming, pl.ds(0, plane - 1), u),
            send_sem=xs.at[u],
            recv_sem=xr.at[u],
            device_id=device(layer, spot + 1),
            device_id_type=MESH,
        )

    produce(0)
    pl.semaphore_wait(barrier, plane + layers + n_sa - 3)
    copy_beside().start()
    for r in range(1, layers):
        route_copy(r).start()
    produce(1)
    copy_beside().wait_recv()
    for r in range(1, plane // 2):
        copy_x(r).start()
    ship(0)

    @pl.loop(2, chunks)
    def _(c):
        produce(c)
        ship(c - 1)

    ship(full)
    ship(full + 1)

    for r in range(1, plane // 2):
        copy_x(r).wait_recv()
    for r in range(1, layers):
        copy_z(r).start()
    for r in range(1, layers):
        route_copy(r).wait_recv()

    @pl.loop(0, layers)
    def _(z):
        table = jnp.concatenate([routes[z], jnp.zeros((128 - deep, tokens), F32)], axis=0)
        table = jnp.transpose(table)
        shift = (z * cap - layer * per_layer).astype(F32)
        start = pl.ds(pl.multiple_of(z * tokens, tokens), tokens)
        for k in range(per_layer // 256):
            slot_of = (lax.broadcasted_iota(jnp.int32, (tokens, 256), 1) + k * 256).astype(F32)
            total = jnp.zeros((tokens, 256), F32)
            for i in range(top):
                total += jnp.where(
                    slot_of == table[:, i : i + 1] + shift, table[:, top + i : top + i + 1], 0.0
                )
            mixing[start, k * 256 : (k + 1) * 256] = total.astype(BF)

    gates(decay_ref, rate_ref, gate)
    prepare_heads(0, q_ref, k_ref, gate, mbo, amat, gmat)
    for r in range(1, layers):
        copy_z(r).wait_recv()
    for r in range(1, n_sa):
        copy_y(r).start()
    copy_last(0).start()

    @pl.loop(1, HK // PAIRS)
    def _(step):
        prepare_heads(step, q_ref, k_ref, gate, mbo, amat, gmat)

    def hop(j, s):
        ahead = s < half
        way = sign if ahead else -sign
        c, at, size = span(j)
        return pltpu.make_async_remote_copy(
            src_ref=zout.at[c, s, :, pl.ds(at, size)],
            dst_ref=zin.at[c, s, :, pl.ds(at, size)],
            send_sem=zs.at[j, s],
            recv_sem=zr.at[j, s],
            device_id=device(layer + way, spot),
            device_id_type=MESH,
        )

    def target(s):
        if s < half:
            return (layer + sign * (half - s) + 2 * layers) % layers
        return (layer - sign * (half - 1 - (s - half)) + 2 * layers) % layers

    hops = layers - 1

    def came(j, h):
        hop(j, h).wait_recv()
        c, at, size = span(j)
        return zin[c, h, :, at : at + size].astype(F32)

    def stage(j, s):
        c, at, size = span(j)
        sent = [h for h in (s, s + half) if h < hops]
        for h in sent:
            part = dense[j % 5, target(h), :, :size]
            if s > 0:
                part = part + came(j, h - 1)
            zout[c, h, :, at : at + size] = part.astype(BF)
        for h in sent:
            hop(j, h).start()

    def last(j):
        c, at, size = span(j)
        total = dense[j % 5, layer, :, :size] + came(j, half - 1) + came(j, hops - 1)
        start = c * wide + at
        cols = pl.ds(start if isinstance(c, int) else pl.multiple_of(start, wide), size)
        moe[:, cols] = (res_ref[:, cols].astype(F32) + total).astype(BF)

    def mix_layer(j, z):
        c, at, size = span(j)
        start = pl.ds(pl.multiple_of(z * tokens, tokens), tokens)
        rowsin = incoming[:, c, :, at : at + size].reshape(per_layer, size)
        dense[j % 5, z, :, :size] = mm(mixing[start, :], rowsin)

    def straight(j, k):
        c, at, size = span(j)
        return pltpu.make_async_remote_copy(
            src_ref=zout.at[c, k - 1, :, pl.ds(at, size)],
            dst_ref=zin.at[c, k - 1, :, pl.ds(at, size)],
            send_sem=zs.at[j, k - 1],
            recv_sem=zr.at[j, k - 1],
            device_id=device(layer + k, spot),
            device_id_type=MESH,
        )

    def arrive_last(j):
        c, at, size = span(j)
        shipped(j).wait_recv()
        order = sorted(range(1, layers), key=lambda k: -min(k, layers - k))
        waiting = []
        for k in order:
            mix_layer(j, (layer + k) % layers)
            zout[c, k - 1, :, at : at + size] = dense[j % 5, (layer + k) % layers, :, :size].astype(BF)
            if waiting:
                straight(j, waiting.pop()).start()
            waiting.append(k)
        mix_layer(j, layer)
        straight(j, waiting.pop()).start()

    def finish_last(j):
        c, at, size = span(j)
        total = dense[j % 5, layer, :, :size]
        for k in range(1, layers):
            straight(j, k).wait_recv()
            total = total + zin[c, k - 1, :, at : at + size].astype(F32)
        cols = pl.ds(c * wide + at, size)
        moe[:, cols] = (res_ref[:, cols].astype(F32) + total).astype(BF)

    def arrive(j):
        shipped(j).wait_recv()
        mix_layer(j, target(0))
        mix_layer(j, target(half))
        stage(j, 0)
        for k in range(layers):
            if k not in (half, half + 1):
                mix_layer(j, (layer + sign * k + 2 * layers) % layers)

    @pl.loop(0, full)
    def _(i):
        @pl.when(i >= half)
        def _():
            last(i - half)

        for s in range(half - 1, 0, -1):

            @pl.when(i >= s)
            def _():
                stage(i - s, s)

        arrive(i)

    for i in range(full, full + 1 + half):
        if i - half < full:
            last(i - half)
        for s in range(half - 1, 0, -1):
            if i - s <= full:
                stage(i - s, s)
        if i == full:
            arrive(i)
        if i == full + 1:
            arrive_last(i)
        if i == full + 2:
            for r in (1, n_sa - 1):
                copy_y(r).wait_recv()
                copy_last(n_sa - r).start()
        if i == full + half:
            for r in range(2, n_sa - 1):
                copy_y(r).wait_recv()
                copy_last(n_sa - r).start()
    last(full)
    finish_last(full + 1)

    stream = moe[...].astype(F32)
    scale = lax.rsqrt(jnp.mean(stream * stream, axis=-1, keepdims=True) + 1e-06)
    stream = stream * scale
    gain = gain_ref[...].astype(F32)
    for g in range(gain.shape[0]):
        cols = slice(g * 128, (g + 1) * 128)
        moe[:, cols] = (stream[:, cols] * gain[g : g + 1]).astype(BF)
    for q in range(n_sa):
        landed(q).wait_recv()

    pair = part // DV

    def pass_on(at):
        return pltpu.make_async_remote_copy(
            src_ref=later.at[at], dst_ref=earlier.at[at], send_sem=ss.at[at], recv_sem=sr.at[at],
            device_id={"sa": (y + 1) % n_sa}, device_id_type=MESH,
        )

    strips = weight.shape[0]

    @pl.loop(0, strips)
    def _(b):
        values = mm(moe[...], weight[b]).astype(BF)
        for h in range(pair):
            both = mm(mbo[b * pair + h], values[:, h * DV : (h + 1) * DV])
            both = both[: 2 * tokens] + both[2 * tokens :]
            fresh[b * pair + h] = both

        @pl.when(y == 0)
        def _():
            for h in range(pair):
                later[b * pair + h] = fresh[b * pair + h, tokens:].astype(BF)
            for h in range(pair):
                pass_on(b * pair + h).start()

    @pl.loop(0, strips)
    def _(b):
        cols = pl.ds(pl.multiple_of(b * part, part), part)

        @pl.when(y == 0)
        def _():
            parts = [fresh[b * pair + h, :tokens] for h in range(pair)]
            out_ref[:, cols] = jnp.concatenate(parts, axis=1).astype(BF)

        @pl.when(y > 0)
        def _():
            for h in range(pair):
                at = b * pair + h
                pass_on(at).wait_recv()

                @pl.when(y < n_sa - 1)
                def _():
                    later[at] = (mm(amat[at], earlier[at]) + fresh[at, tokens:]).astype(BF)
                    pass_on(at).start()

            parts = [
                fresh[b * pair + h, :tokens] + mm(gmat[b * pair + h], earlier[b * pair + h]) for h in range(pair)
            ]
            out_ref[:, cols] = jnp.concatenate(parts, axis=1).astype(BF)

    @pl.when(y < n_sa - 1)
    def _():
        for at in range(strips * pair):
            pass_on(at).wait_send()

    copy_beside().wait_send()
    for r in range(1, plane // 2):
        copy_x(r).wait_send()
    for r in range(1, layers):
        copy_z(r).wait_send()
    for r in range(1, n_sa):
        copy_y(r).wait_send()
    for q in range(n_sa):
        copy_last(q).wait_send()
    for r in range(1, layers):
        route_copy(r).wait_send()

    def drained(u):
        shipped(u).wait_send()
        for s in range(hops):
            hop(u, s).wait_send()

    @pl.loop(0, full)
    def _(u):
        drained(u)

    drained(full)
    shipped(full + 1).wait_send()
    for k in range(1, layers):
        straight(full + 1, k).wait_send()


def layer(
    plane, expert_hidden, down_weight, residual, ids, amount, gain, value_weight, queries, keys, decay, rate
):
    exp_dev, rows, ff_units = expert_hidden.shape
    width = down_weight.shape[2]
    n_ea = lax.axis_size("ea")
    n_sa = lax.axis_size("sa")
    layers = n_ea // plane
    cap = rows // n_ea
    top, _, tokens = ids.shape
    wide = 256
    chunks = width // wide
    block = exp_dev * layers * cap
    source = np.arange(rows).reshape(layers, plane, cap).transpose(1, 0, 2).reshape(-1)
    order = np.zeros((rows, rows), np.float32)
    order[np.arange(rows), source] = 1.0
    strips = 2 * n_sa
    part = width // strips
    vmem = pl.BlockSpec(memory_space=pltpu.VMEM)
    hbm = pl.BlockSpec(memory_space=pl.ANY)
    dma = pltpu.SemaphoreType.DMA
    return pl.pallas_call(
        functools.partial(layer_kernel, plane, layers),
        out_shape=jax.ShapeDtypeStruct((tokens, width), BF),
        in_specs=[vmem, hbm] + [vmem] * 10,
        out_specs=vmem,
        scratch_shapes=[
            pltpu.VMEM((exp_dev, rows, ff_units), BF),
            pltpu.VMEM((3, exp_dev, ff_units, wide), BF),
            pltpu.VMEM((plane, chunks, block, wide), BF),
            pltpu.VMEM((plane, chunks, block, wide), BF),
            pltpu.VMEM((layers * tokens, plane * block), BF),
            pltpu.VMEM((5, layers, tokens, wide), F32),
            pltpu.VMEM((chunks, layers - 1, tokens, wide), BF),
            pltpu.VMEM((chunks, layers - 1, tokens, wide), BF),
            pltpu.VMEM((layers, 24, tokens), F32),
            pltpu.VMEM((tokens, width), BF),
            pltpu.VMEM((strips, width, part), BF),
            pltpu.VMEM((HV, 4 * tokens, tokens), BF),
            pltpu.VMEM((HV, DK, DK), BF),
            pltpu.VMEM((HV, tokens, DK), BF),
            pltpu.VMEM((4, tokens, 128), F32),
            pltpu.VMEM((HV, tokens + DK, DV), F32),
            pltpu.VMEM((HV, DK, DV), BF),
            pltpu.VMEM((HV, DK, DV), BF),
            dma((3,)),
            dma((chunks + 1,)),
            dma((chunks + 1,)),
            dma((chunks + 1, layers - 1)),
            dma((chunks + 1, layers - 1)),
            dma((layers,)),
            dma((layers,)),
            dma((18,)),
            dma((18,)),
            dma((HV,)),
            dma((HV,)),
        ],
        compiler_params=pltpu.CompilerParams(
            collective_id=0, has_side_effects=True, vmem_limit_bytes=63 * 1024 * 1024
        ),
        cost_estimate=pl.CostEstimate(flops=60_000_000_000, bytes_accessed=12_000_000, transcendentals=0),
        name="layer",
    )(
        expert_hidden, down_weight, jnp.asarray(order, BF), ids, amount, residual,
        gain.reshape(width // 128, 128), value_weight, queries, keys, decay, rate,
    )


def solution(mesh):
    def body(
        expert_hidden, down_weight, residual, expert_ids, combine_weight, norm_gain, value_weight,
        queries, keys, log_decay, write_rate,
    ):
        return layer(
            8, expert_hidden, down_weight, residual[0], expert_ids.transpose(2, 0, 1),
            combine_weight.transpose(2, 0, 1), norm_gain, value_weight, queries[0], keys[0],
            log_decay[0].T, write_rate[0].T,
        )[None]

    return jax.shard_map(
        body,
        mesh=mesh,
        in_specs=(
            P("ea", "sa", None),
            P("ea", None, None),
            P("ea", "sa", None),
            P("ea", "sa", None),
            P("ea", "sa", None),
            P(),
            P("ea", None),
            P("ea", "sa", None),
            P("ea", "sa", None),
            P("ea", "sa", None),
            P("ea", "sa", None),
        ),
        out_specs=P("ea", "sa", None),
        check_vma=False,
    )
```

```python
import functools

import jax
import jax.numpy as jnp
import numpy as np
from jax import lax
from jax.experimental import pallas as pl
from jax.experimental.pallas import tpu as pltpu
from jax.sharding import PartitionSpec as P

HV = 16
HK = 8
DK = 128
DV = 128
BF = jnp.bfloat16
F32 = jnp.float32
MESH = pl.DeviceIdType.MESH


def mm(a, b, dims=((1,), (0,))):
    return lax.dot_general(a.astype(BF), b.astype(BF), (dims, ((), ())), preferred_element_type=F32)


def mm_full(a, b, dims=((1,), (0,))):
    return lax.dot_general(
        a, b, (dims, ((), ())), preferred_element_type=F32, precision=lax.Precision.HIGHEST
    )


def mm3(a, b):
    ah, bh = a.astype(BF), b.astype(BF)
    al = (a - ah.astype(F32)).astype(BF)
    bl = (b - bh.astype(F32)).astype(BF)
    return mm(ah, bh) + (mm(ah, bl) + mm(al, bh))


def unit_lower_inverses(lowers):
    n = lowers[0].shape[0]
    row = lax.broadcasted_iota(jnp.int32, (n, n), 0)
    col = lax.broadcasted_iota(jnp.int32, (n, n), 1)
    eye = (row == col).astype(F32)
    size = 16
    same = (row // size) == (col // size)
    powers = [jnp.where(same, -low, 0.0) for low in lowers]
    outs = [eye + p for p in powers]
    for _ in range(3):
        powers = [mm3(p, p) for p in powers]
        outs = [o + mm3(p, o) for p, o in zip(powers, outs)]
    while size < n:
        join = ((row // (2 * size)) == (col // (2 * size))) & ((row // size) > (col // size))
        parts = [mm3(jnp.where(join, low, 0.0), o) for low, o in zip(lowers, outs)]
        outs = [o - mm3(o, p) for o, p in zip(outs, parts)]
        size *= 2
    return outs


PAIRS = 4


def gates(decay_ref, rate_ref, gate):
    heads, n = decay_ref.shape
    row = lax.broadcasted_iota(jnp.int32, (n, n), 0)
    col = lax.broadcasted_iota(jnp.int32, (n, n), 1)
    blank = jnp.zeros((n - heads, n), F32)
    summed = mm_full(decay_ref[...], jnp.where(row <= col, 1.0, 0.0))
    for at, rows in ((0, summed), (2, rate_ref[...])):
        rows = jnp.concatenate([rows, blank], axis=0)
        gate[at] = jnp.transpose(rows)
        gate[at + 1] = rows


def prepare_heads(step, q_ref, k_ref, gate, mbo_ref, a_ref, g_ref):
    pairs = PAIRS
    n = q_ref.shape[0]
    row = lax.broadcasted_iota(jnp.int32, (n, n), 0)
    col = lax.broadcasted_iota(jnp.int32, (n, n), 1)
    inclusive = row >= col
    strict = row > col
    eye = (row == col).astype(F32)
    ones = jnp.ones((8, DK), F32)
    base = step * (2 * pairs)
    heads, lowers = [], []
    wide = pl.ds(pl.multiple_of(step * (pairs * DK), pairs * DK), pairs * DK)
    all_q, all_k = q_ref[:, wide], k_ref[:, wide]
    these = pl.ds(pl.multiple_of(base, 2 * pairs), 2 * pairs)
    sum_rows, rate_rows = gate[1, these], gate[3, these]
    for pair in range(pairs):
        q = all_q[:, pair * DK : (pair + 1) * DK]
        k = all_k[:, pair * DK : (pair + 1) * DK]
        qf, kf = q.astype(F32), k.astype(F32)
        kn_col = lax.rsqrt(jnp.sum(kf * kf, axis=-1, keepdims=True) + 1e-06)
        qn_col = lax.rsqrt(jnp.sum(qf * qf, axis=-1, keepdims=True) + 1e-06) * DK ** (-0.5)
        kn_row = lax.rsqrt(mm_full(ones, kf * kf, ((1,), (1,)))[:1] + 1e-06)
        kk = mm(k, k, ((1,), (1,))) * kn_col * kn_row
        qk = mm(q, k, ((1,), (1,))) * qn_col * kn_row
        for half in range(2):
            h = 2 * pair + half
            pick = col == base + h
            g_col = jnp.sum(jnp.where(pick, gate[0], 0.0), axis=1, keepdims=True)
            rate_col = jnp.sum(jnp.where(pick, gate[2], 0.0), axis=1, keepdims=True)
            g_row = sum_rows[h : h + 1, :]
            rate_row = rate_rows[h : h + 1, :]
            ratio = jnp.where(inclusive, jnp.exp(jnp.where(inclusive, g_col - g_row, 0.0)), 0.0)
            lowers.append(jnp.where(strict, rate_col * ratio * kk, 0.0))
            heads.append((h, q, k, qf, kf, kn_col, qn_col, kn_row, g_col, g_row, rate_row, qk * ratio))
    inverses = unit_lower_inverses(lowers)
    for inverse, (h, q, k, qf, kf, kn_col, qn_col, kn_row, g_col, g_row, rate_row, scores) in zip(inverses, heads):
        mix = inverse * rate_row
        emat = mm(mix * (jnp.exp(g_row) * kn_row), k)
        last = g_col[n - 1 : n, :]
        ktail = kf * (kn_col * jnp.exp(last - g_col))
        a_ref[base + h] = (jnp.exp(last) * eye - mm(ktail, emat, ((0,), (0,)))).astype(BF)
        for at, part in ((0, mm3(scores, mix)), (n, mm3(jnp.transpose(ktail), mix))):
            high = part.astype(BF)
            mbo_ref[base + h, at : at + n, :] = high
            mbo_ref[base + h, 2 * n + at : 3 * n + at, :] = (part - high.astype(F32)).astype(BF)
        g_ref[base + h] = (jnp.exp(g_col) * qn_col * qf - mm(scores, emat)).astype(BF)


def layer_kernel(
    plane, layers, hid_ref, down_ref, order_ref, ids_ref, amount_ref, res_ref, gain_ref, value_ref,
    q_ref, k_ref, decay_ref, rate_ref, out_ref,
    hidden, down, outgoing, incoming, mixing, dense, zout, zin, routes, moe,
    weight, mbo, amat, gmat, gate, fresh, later, earlier,
    dsem, xs, xr, zs, zr, rs, rr, ws, wr, ss, sr,
):
    exp_dev, rows, _ = hid_ref.shape
    top, _, tokens = ids_ref.shape
    _, chunks, block, wide = outgoing.shape
    full = chunks - 1
    units = chunks + 1

    def span(u):
        if isinstance(u, int) and u >= full:
            return full, (u - full) * (wide // 2), wide // 2
        return u, 0, wide
    cap = rows // (plane * layers)
    group = layers * cap
    per_layer = plane * block
    me = lax.axis_index("ea")
    spot, layer = me % plane, me // plane
    sign = 1 - 2 * (me % 2)
    half = layers // 2

    y = lax.axis_index("sa")
    n_sa = lax.axis_size("sa")
    core = me % 2
    strip = y * 2 + core
    near = spot // 2

    def chunk_copy(c):
        at = pl.ds(pl.multiple_of(c * wide, wide), wide)
        return pltpu.make_async_copy(down_ref.at[:, :, at], down.at[c % depth], dsem.at[c % depth])

    depth = down.shape[0]
    for c in range(depth):
        chunk_copy(c).start()

    def device(z, p):
        return {"ea": ((z + 2 * layers) % layers) * plane + p % plane}

    barrier = pltpu.get_barrier_semaphore()
    for r in range(1, plane):
        pl.semaphore_signal(barrier, inc=1, device_id=device(layer, spot + r), device_id_type=MESH)
    for r in range(1, layers):
        pl.semaphore_signal(barrier, inc=1, device_id=device(layer + r, spot), device_id_type=MESH)
    for r in range(1, n_sa):
        pl.semaphore_signal(barrier, inc=1, device_id={"sa": (y + r) % n_sa}, device_id_type=MESH)

    own_rows, part = value_ref.shape[0], weight.shape[2]

    def remote(src, dst, at, to):
        return pltpu.make_async_remote_copy(
            src_ref=src, dst_ref=dst, send_sem=ws.at[at], recv_sem=wr.at[at],
            device_id=to, device_id_type=MESH,
        )

    def weight_rows(start, size):
        return weight.at[strip, pl.ds(pl.multiple_of(start * size, size), size)]

    def copy_beside():
        other = y * 2 + 1 - core
        cols = pl.ds(pl.multiple_of(other * part, part), part)
        mine = pl.ds(pl.multiple_of(me * own_rows, own_rows), own_rows)
        return remote(value_ref.at[:, cols], weight.at[other, mine], 0, {"ea": me + 1 - 2 * core})

    def copy_x(r):
        ref = weight_rows(me // 2, 2 * own_rows)
        return remote(ref, ref, r, device(layer, ((near + r) % (plane // 2)) * 2 + core))

    def copy_z(r):
        ref = weight_rows(layer, plane * own_rows)
        return remote(ref, ref, 3 + r, device(layer + r, spot))

    def copy_y(r):
        return remote(weight.at[strip], weight.at[strip], 10 + r, {"sa": (y + r) % n_sa})

    def copy_last(q):
        ref = weight.at[((y + q) % n_sa) * 2 + core]
        return remote(ref, ref, 14 + (y + q) % n_sa, {"ea": me + 1 - 2 * core})

    def landed(q):
        ref = weight.at[((y + q) % n_sa) * 2 + 1 - core]
        return remote(ref, ref, 14 + (y + q) % n_sa, {"ea": me + 1 - 2 * core})

    weight[strip, pl.ds(pl.multiple_of(me * own_rows, own_rows), own_rows)] = value_ref[
        :, pl.ds(pl.multiple_of(strip * part, part), part)
    ]

    experts = exp_dev * plane * layers
    name = lax.broadcasted_iota(jnp.int32, (experts, tokens), 0)
    counts = jnp.zeros((experts, tokens), F32)
    for i in range(top):
        counts += jnp.where(name == ids_ref[i], 1.0, 0.0)
    trow = lax.broadcasted_iota(jnp.int32, (tokens, tokens), 0)
    tcol = lax.broadcasted_iota(jnp.int32, (tokens, tokens), 1)
    prior = mm(counts, jnp.where(trow < tcol, 1.0, 0.0))
    found = []
    for i in range(top):
        ids = ids_ref[i]
        slot = jnp.sum(jnp.where(name == ids, prior, 0.0), axis=0, keepdims=True)
        place = (ids // exp_dev) * block + (ids % exp_dev) * group
        found.append(place.astype(F32) + slot)
    found += [amount_ref[i] for i in range(top)]
    deep = routes.shape[1]
    found.append(jnp.zeros((deep - 2 * top, tokens), F32))
    routes[layer] = jnp.concatenate(found, axis=0)

    for e in range(exp_dev):
        hidden[e] = mm(order_ref[...], hid_ref[e]).astype(BF)

    def route_copy(r):
        return pltpu.make_async_remote_copy(
            src_ref=routes.at[layer],
            dst_ref=routes.at[layer],
            send_sem=rs.at[r],
            recv_sem=rr.at[r],
            device_id=device(layer + r, spot),
            device_id_type=MESH,
        )

    def produce(c):
        chunk_copy(c).wait()
        made = [mm(hidden[e], down[c % depth, e]) for e in range(exp_dev)]
        for p in range(plane):
            mine = [m[p * group : (p + 1) * group] for m in made]
            outgoing[p, c] = jnp.concatenate(mine, axis=0).astype(BF)

        @pl.when(c + depth < chunks)
        def _():
            chunk_copy(c + depth).start()

    def block_of(ref, p, u):
        c, at, size = span(u)
        return ref.at[p, c, :, pl.ds(at, size)]

    def ship(u):
        def send(to):
            pltpu.make_async_remote_copy(
                src_ref=block_of(outgoing, to, u),
                dst_ref=block_of(incoming, spot, u),
                send_sem=xs.at[u],
                recv_sem=xr.at[u],
                device_id=device(layer, to),
                device_id_type=MESH,
            ).start()

        for c in range(2):
            for dx in (2, 1, 3):
                send(((near + sign * dx + plane) % (plane // 2)) * 2 + c)
        send(spot + 1 - 2 * core)
        c, at, size = span(u)
        incoming[spot, c, :, at : at + size] = outgoing[spot, c, :, at : at + size]

    def shipped(u):
        return pltpu.make_async_remote_copy(
            src_ref=block_of(outgoing, pl.ds(0, plane - 1), u),
            dst_ref=block_of(incoming, pl.ds(0, plane - 1), u),
            send_sem=xs.at[u],
            recv_sem=xr.at[u],
            device_id=device(layer, spot + 1),
            device_id_type=MESH,
        )

    produce(0)
    pl.semaphore_wait(barrier, plane + layers + n_sa - 3)
    copy_beside().start()
    for r in range(1, layers):
        route_copy(r).start()
    produce(1)
    copy_beside().wait_recv()
    for r in range(1, plane // 2):
        copy_x(r).start()
    ship(0)

    @pl.loop(2, chunks // 2 + 1)
    def _(c):
        produce(c)
        ship(c - 1)

    for r in range(1, plane // 2):
        copy_x(r).wait_recv()
    for r in range(1, layers):
        copy_z(r).start()

    @pl.loop(chunks // 2 + 1, chunks)
    def _(c):
        produce(c)
        ship(c - 1)

    ship(full)
    ship(full + 1)

    for r in range(1, layers):
        route_copy(r).wait_recv()

    @pl.loop(0, layers)
    def _(z):
        table = jnp.concatenate([routes[z], jnp.zeros((128 - deep, tokens), F32)], axis=0)
        table = jnp.transpose(table)
        shift = (z * cap - layer * per_layer).astype(F32)
        start = pl.ds(pl.multiple_of(z * tokens, tokens), tokens)
        for k in range(per_layer // 256):
            slot_of = (lax.broadcasted_iota(jnp.int32, (tokens, 256), 1) + k * 256).astype(F32)
            total = jnp.zeros((tokens, 256), F32)
            for i in range(top):
                total += jnp.where(
                    slot_of == table[:, i : i + 1] + shift, table[:, top + i : top + i + 1], 0.0
                )
            mixing[start, k * 256 : (k + 1) * 256] = total.astype(BF)

    gates(decay_ref, rate_ref, gate)
    prepare_heads(0, q_ref, k_ref, gate, mbo, amat, gmat)
    for r in range(1, layers):
        copy_z(r).wait_recv()
    for r in range(1, n_sa):
        copy_y(r).start()
    copy_last(0).start()

    @pl.loop(1, HK // PAIRS)
    def _(step):
        prepare_heads(step, q_ref, k_ref, gate, mbo, amat, gmat)

    def hop(j, s):
        ahead = s < half
        way = sign if ahead else -sign
        c, at, size = span(j)
        return pltpu.make_async_remote_copy(
            src_ref=zout.at[c, s, :, pl.ds(at, size)],
            dst_ref=zin.at[c, s, :, pl.ds(at, size)],
            send_sem=zs.at[j, s],
            recv_sem=zr.at[j, s],
            device_id=device(layer + way, spot),
            device_id_type=MESH,
        )

    def target(s):
        if s < half:
            return (layer + sign * (half - s) + 2 * layers) % layers
        return (layer - sign * (half - 1 - (s - half)) + 2 * layers) % layers

    hops = layers - 1

    def came(j, h):
        hop(j, h).wait_recv()
        c, at, size = span(j)
        return zin[c, h, :, at : at + size].astype(F32)

    def stage(j, s):
        c, at, size = span(j)
        sent = [h for h in (s, s + half) if h < hops]
        for h in sent:
            part = dense[j % 5, target(h), :, :size]
            if s > 0:
                part = part + came(j, h - 1)
            zout[c, h, :, at : at + size] = part.astype(BF)
        for h in sent:
            hop(j, h).start()

    def last(j):
        c, at, size = span(j)
        total = dense[j % 5, layer, :, :size] + came(j, half - 1) + came(j, hops - 1)
        start = c * wide + at
        cols = pl.ds(start if isinstance(c, int) else pl.multiple_of(start, wide), size)
        moe[:, cols] = (res_ref[:, cols].astype(F32) + total).astype(BF)

    def mix_layer(j, z):
        c, at, size = span(j)
        start = pl.ds(pl.multiple_of(z * tokens, tokens), tokens)
        rowsin = incoming[:, c, :, at : at + size].reshape(per_layer, size)
        dense[j % 5, z, :, :size] = mm(mixing[start, :], rowsin)

    def straight(j, k):
        c, at, size = span(j)
        return pltpu.make_async_remote_copy(
            src_ref=zout.at[c, k - 1, :, pl.ds(at, size)],
            dst_ref=zin.at[c, k - 1, :, pl.ds(at, size)],
            send_sem=zs.at[j, k - 1],
            recv_sem=zr.at[j, k - 1],
            device_id=device(layer + k, spot),
            device_id_type=MESH,
        )

    def arrive_last(j):
        c, at, size = span(j)
        shipped(j).wait_recv()
        order = sorted(range(1, layers), key=lambda k: -min(k, layers - k))
        waiting = []
        for k in order:
            mix_layer(j, (layer + k) % layers)
            zout[c, k - 1, :, at : at + size] = dense[j % 5, (layer + k) % layers, :, :size].astype(BF)
            if waiting:
                straight(j, waiting.pop()).start()
            waiting.append(k)
        mix_layer(j, layer)
        straight(j, waiting.pop()).start()

    def finish_last(j):
        c, at, size = span(j)
        total = dense[j % 5, layer, :, :size]
        for k in range(1, layers):
            straight(j, k).wait_recv()
            total = total + zin[c, k - 1, :, at : at + size].astype(F32)
        cols = pl.ds(c * wide + at, size)
        moe[:, cols] = (res_ref[:, cols].astype(F32) + total).astype(BF)

    def arrive(j):
        shipped(j).wait_recv()
        mix_layer(j, target(0))
        mix_layer(j, target(half))
        stage(j, 0)
        for k in range(layers):
            if k not in (half, half + 1):
                mix_layer(j, (layer + sign * k + 2 * layers) % layers)

    @pl.loop(0, full)
    def _(i):
        @pl.when(i >= half)
        def _():
            last(i - half)

        for s in range(half - 1, 0, -1):

            @pl.when(i >= s)
            def _():
                stage(i - s, s)

        arrive(i)

    for i in range(full, full + 1 + half):
        if i - half < full:
            last(i - half)
        for s in range(half - 1, 0, -1):
            if i - s <= full:
                stage(i - s, s)
        if i == full:
            arrive(i)
        if i == full + 1:
            arrive_last(i)
        if i == full + 2:
            for r in (1, n_sa - 1):
                copy_y(r).wait_recv()
                copy_last(n_sa - r).start()
        if i == full + half:
            for r in range(2, n_sa - 1):
                copy_y(r).wait_recv()
                copy_last(n_sa - r).start()
    last(full)
    finish_last(full + 1)

    stream = moe[...].astype(F32)
    scale = lax.rsqrt(jnp.mean(stream * stream, axis=-1, keepdims=True) + 1e-06)
    stream = stream * scale
    gain = gain_ref[...].astype(F32)
    for g in range(gain.shape[0]):
        cols = slice(g * 128, (g + 1) * 128)
        moe[:, cols] = (stream[:, cols] * gain[g : g + 1]).astype(BF)
    for q in range(n_sa):
        landed(q).wait_recv()

    pair = part // DV

    def pass_on(at):
        return pltpu.make_async_remote_copy(
            src_ref=later.at[at], dst_ref=earlier.at[at], send_sem=ss.at[at], recv_sem=sr.at[at],
            device_id={"sa": (y + 1) % n_sa}, device_id_type=MESH,
        )

    strips = weight.shape[0]

    @pl.loop(0, strips)
    def _(b):
        values = mm(moe[...], weight[b]).astype(BF)
        for h in range(pair):
            both = mm(mbo[b * pair + h], values[:, h * DV : (h + 1) * DV])
            both = both[: 2 * tokens] + both[2 * tokens :]
            fresh[b * pair + h] = both

        @pl.when(y == 0)
        def _():
            for h in range(pair):
                later[b * pair + h] = fresh[b * pair + h, tokens:].astype(BF)
            for h in range(pair):
                pass_on(b * pair + h).start()

    @pl.loop(0, strips)
    def _(b):
        cols = pl.ds(pl.multiple_of(b * part, part), part)

        @pl.when(y == 0)
        def _():
            parts = [fresh[b * pair + h, :tokens] for h in range(pair)]
            out_ref[:, cols] = jnp.concatenate(parts, axis=1).astype(BF)

        @pl.when(y > 0)
        def _():
            for h in range(pair):
                at = b * pair + h
                pass_on(at).wait_recv()

                @pl.when(y < n_sa - 1)
                def _():
                    later[at] = (mm(amat[at], earlier[at]) + fresh[at, tokens:]).astype(BF)
                    pass_on(at).start()

            parts = [
                fresh[b * pair + h, :tokens] + mm(gmat[b * pair + h], earlier[b * pair + h]) for h in range(pair)
            ]
            out_ref[:, cols] = jnp.concatenate(parts, axis=1).astype(BF)

    @pl.when(y < n_sa - 1)
    def _():
        for at in range(strips * pair):
            pass_on(at).wait_send()

    copy_beside().wait_send()
    for r in range(1, plane // 2):
        copy_x(r).wait_send()
    for r in range(1, layers):
        copy_z(r).wait_send()
    for r in range(1, n_sa):
        copy_y(r).wait_send()
    for q in range(n_sa):
        copy_last(q).wait_send()
    for r in range(1, layers):
        route_copy(r).wait_send()

    def drained(u):
        shipped(u).wait_send()
        for s in range(hops):
            hop(u, s).wait_send()

    @pl.loop(0, full)
    def _(u):
        drained(u)

    drained(full)
    shipped(full + 1).wait_send()
    for k in range(1, layers):
        straight(full + 1, k).wait_send()


def layer(
    plane, expert_hidden, down_weight, residual, ids, amount, gain, value_weight, queries, keys, decay, rate
):
    exp_dev, rows, ff_units = expert_hidden.shape
    width = down_weight.shape[2]
    n_ea = lax.axis_size("ea")
    n_sa = lax.axis_size("sa")
    layers = n_ea // plane
    cap = rows // n_ea
    top, _, tokens = ids.shape
    wide = 256
    chunks = width // wide
    block = exp_dev * layers * cap
    source = np.arange(rows).reshape(layers, plane, cap).transpose(1, 0, 2).reshape(-1)
    order = np.zeros((rows, rows), np.float32)
    order[np.arange(rows), source] = 1.0
    strips = 2 * n_sa
    part = width // strips
    vmem = pl.BlockSpec(memory_space=pltpu.VMEM)
    hbm = pl.BlockSpec(memory_space=pl.ANY)
    dma = pltpu.SemaphoreType.DMA
    return pl.pallas_call(
        functools.partial(layer_kernel, plane, layers),
        out_shape=jax.ShapeDtypeStruct((tokens, width), BF),
        in_specs=[vmem, hbm] + [vmem] * 10,
        out_specs=vmem,
        scratch_shapes=[
            pltpu.VMEM((exp_dev, rows, ff_units), BF),
            pltpu.VMEM((3, exp_dev, ff_units, wide), BF),
            pltpu.VMEM((plane, chunks, block, wide), BF),
            pltpu.VMEM((plane, chunks, block, wide), BF),
            pltpu.VMEM((layers * tokens, plane * block), BF),
            pltpu.VMEM((5, layers, tokens, wide), F32),
            pltpu.VMEM((chunks, layers - 1, tokens, wide), BF),
            pltpu.VMEM((chunks, layers - 1, tokens, wide), BF),
            pltpu.VMEM((layers, 24, tokens), F32),
            pltpu.VMEM((tokens, width), BF),
            pltpu.VMEM((strips, width, part), BF),
            pltpu.VMEM((HV, 4 * tokens, tokens), BF),
            pltpu.VMEM((HV, DK, DK), BF),
            pltpu.VMEM((HV, tokens, DK), BF),
            pltpu.VMEM((4, tokens, 128), F32),
            pltpu.VMEM((HV, tokens + DK, DV), F32),
            pltpu.VMEM((HV, DK, DV), BF),
            pltpu.VMEM((HV, DK, DV), BF),
            dma((3,)),
            dma((chunks + 1,)),
            dma((chunks + 1,)),
            dma((chunks + 1, layers - 1)),
            dma((chunks + 1, layers - 1)),
            dma((layers,)),
            dma((layers,)),
            dma((18,)),
            dma((18,)),
            dma((HV,)),
            dma((HV,)),
        ],
        compiler_params=pltpu.CompilerParams(
            collective_id=0, has_side_effects=True, vmem_limit_bytes=63 * 1024 * 1024
        ),
        cost_estimate=pl.CostEstimate(flops=60_000_000_000, bytes_accessed=12_000_000, transcendentals=0),
        name="layer",
    )(
        expert_hidden, down_weight, jnp.asarray(order, BF), ids, amount, residual,
        gain.reshape(width // 128, 128), value_weight, queries, keys, decay, rate,
    )


def solution(mesh):
    def body(
        expert_hidden, down_weight, residual, expert_ids, combine_weight, norm_gain, value_weight,
        queries, keys, log_decay, write_rate,
    ):
        return layer(
            8, expert_hidden, down_weight, residual[0], expert_ids.transpose(2, 0, 1),
            combine_weight.transpose(2, 0, 1), norm_gain, value_weight, queries[0], keys[0],
            log_decay[0].T, write_rate[0].T,
        )[None]

    return jax.shard_map(
        body,
        mesh=mesh,
        in_specs=(
            P("ea", "sa", None),
            P("ea", None, None),
            P("ea", "sa", None),
            P("ea", "sa", None),
            P("ea", "sa", None),
            P(),
            P("ea", None),
            P("ea", "sa", None),
            P("ea", "sa", None),
            P("ea", "sa", None),
            P("ea", "sa", None),
        ),
        out_specs=P("ea", "sa", None),
        check_vma=False,
    )
```
